32 devices in a mesh: rve: 4 (over z), mic: 4 (over y, x), mac: 2 (over core).
Axes of the slice: x: 2, y: 2, z: 4, core: 2. Of those that a mesh axis runs over, the one named last changes fastest.
Arguments:
- displacement: float32 [3, 4, 8, 8], P(None, 'rve', ('mic', 'mac')), may hold values from -3 to 3
- plastic: float32 [256, 6, 16, 256], P(('rve', 'mic', 'mac')), may hold values from -0.3 to 0.3
- bulk_modulus: float32 [16, 256], replicated, may hold values from 1 to 3
- shear_modulus: float32 [16, 256], replicated, may hold values from 0.5 to 1.5
- yield_radius: float32 [16, 256], replicated, may hold values from 0.05 to 0.3
- counts: int32 [256], P(('rve', 'mic', 'mac')), may hold values from 0 to 3
- migration_plan: int32 [256], P(('rve', 'mic', 'mac')), may hold values from 0 to 255, as said below
Outputs:
- nodal_force: float32 [3, 4, 8, 8], P(None, 'rve', ('mic', 'mac'))
- plastic_new: float32 [256, 6, 16, 256], P(('rve', 'mic', 'mac'))
The draws below stay inside these ranges and needn't reach their ends.
Inputs may be any that keep to these rules, and one draw needn't show every extreme that they name: migration_plan is a permutation of 0 .. 255. It keeps an RVE within the devices that share its mic and mac index; each device sends exactly 4 of its RVEs to each of 2 devices along rve and none to the others, so that every device receives 8. At each receiving device the RVEs are placed in order of rising iteration count.
All inputs are finite; a program needn't handle non-finite values.
Results may differ from the reference program's by a relative error of at most 0.0003.
Values sent between devices are 32-bit elements; how exact they have to be, the bound alone decides.
No kernel may reach another device: no remote copies, remote signals or barrier semaphores. Data moves between devices by JAX's collectives and lax.ppermute only.
A program may use at most 128 MiB of HBM per device.

```python
import math
import jax
import jax.numpy as jnp
from jax import lax

G = 16
ITER_PEAK = 3
RBLK = 4
NZ = 8
R_LOC = 8
NX = 4
NY = 8
NE = 256
PEERS = 2
CAP = 4
N_RVE = 4
N_MIC = 4
N_MAC = 2


def plan_parts(key):
    folded = jax.random.fold_in(key, 4242)
    subkeys = jax.random.split(folded, 7)
    columns = N_MIC * N_MAC
    groups_total = N_RVE * columns
    loaded = jax.random.randint(subkeys[0], (N_RVE, columns), 0, 4) == 0
    forced = jax.random.randint(subkeys[1], (), 0, groups_total)
    loaded = loaded | (jnp.arange(groups_total).reshape(N_RVE, columns) == forced)
    upper_draw = jax.random.randint(subkeys[2], (N_RVE, columns, R_LOC), 1, ITER_PEAK + 1)
    lower_draw = jax.random.randint(subkeys[3], (N_RVE, columns, R_LOC), 0, 2)
    iterations = jnp.where(loaded[:, :, None], upper_draw, lower_draw)
    first_slot = (jnp.arange(R_LOC) == 0)[None, None, :]
    iterations = jnp.where(loaded[:, :, None] & first_slot, ITER_PEAK, iterations)
    offset_index = jnp.arange(N_RVE)
    offset_score = jax.random.randint(subkeys[4], (N_RVE,), 0, 2 ** 16) * N_RVE + offset_index
    required = (offset_index == 1) | (offset_index == N_RVE // 2)
    offset_score = jnp.where(required, offset_index - 2 * N_RVE, offset_score)
    offsets = jnp.argsort(offset_score)[:PEERS].astype(jnp.int32)
    shuffle = jax.random.randint(subkeys[5], (N_RVE, columns, R_LOC), 0, 2 ** 16) * R_LOC + jnp.arange(R_LOC)[None, None, :]
    position = jnp.argsort(jnp.argsort(shuffle, axis=-1), axis=-1)
    bundle = position // CAP
    target = (jnp.arange(N_RVE)[:, None, None] + offsets[bundle]) % N_RVE
    flat_index = jnp.arange(N_RVE)[:, None, None] * R_LOC + jnp.arange(R_LOC)[None, None, :]
    tiebreak = jax.random.randint(subkeys[6], (N_RVE, columns, R_LOC), 0, 2 ** 12) * (N_RVE * R_LOC) + flat_index
    ordering = iterations * (2 ** 12 * N_RVE * R_LOC) + tiebreak
    target_cols = jnp.transpose(target, (1, 0, 2)).reshape(columns, N_RVE * R_LOC)
    ordering_cols = jnp.transpose(ordering, (1, 0, 2)).reshape(columns, N_RVE * R_LOC)
    shared = target_cols[:, :, None] == target_cols[:, None, :]
    smaller = ordering_cols[:, None, :] < ordering_cols[:, :, None]
    arrival = jnp.sum((shared & smaller).astype(jnp.int32), axis=2)
    arrival = jnp.transpose(arrival.reshape(columns, N_RVE, R_LOC), (1, 0, 2))
    destination = (target * columns + jnp.arange(columns)[None, :, None]) * R_LOC + arrival
    return (iterations.reshape(-1).astype(jnp.int32), destination.reshape(-1).astype(jnp.int32))


def draw_counts(key, part):
    return plan_parts(key)[0]


def draw_migration_plan(key, part):
    return plan_parts(key)[1]


def block_levels(own_key, shape, shards, low, high):
    def one(axis_at, blocks):
        heights = jax.random.uniform(jax.random.fold_in(jax.random.fold_in(own_key, 6), axis_at), (blocks,), jnp.float32, low / len(shards), high / len(shards))
        return jnp.repeat(jnp.exp(heights), shape[axis_at] // blocks).reshape((-1,) + (1,) * (len(shape) - axis_at - 1))

    level = one(*shards[0])
    for cut in shards[1:]:
        level = level * one(*cut)
    return level


def normal_values(stream_key, shape, scale, bound, cuts=(), kind=jnp.bfloat16):
    factor_of = block_levels(stream_key, shape, cuts, -0.22, 0.18) if cuts else 1.0
    drawn = jax.random.normal(stream_key, shape, jnp.float32) * scale * factor_of
    return jnp.minimum(jnp.maximum(drawn, -bound), bound).astype(kind)


def setup_inputs(seed: int = 0) -> dict:
    key_list = jax.random.split(jax.random.key(seed), 8)
    return {
        "displacement": normal_values(key_list[0], (3, NX, NY, NZ), 0.5, 3.0, ((1, 4), (2, 8)), jnp.float32),
        "plastic": normal_values(key_list[1], (NE, 6, G, G * G), 0.05, 0.3, ((0, 32),), jnp.float32),
        "bulk_modulus": jnp.clip(jax.random.uniform(key_list[2], (G, G * G), jnp.float32, 1.0, 3.0), 1.0, 3.0),
        "shear_modulus": jnp.clip(jax.random.uniform(key_list[3], (G, G * G), jnp.float32, 0.5, 1.5), 0.5, 1.5),
        "yield_radius": jnp.clip(jnp.exp(jax.random.uniform(key_list[4], (G, G * G), jnp.float32, math.log(0.05), math.log(0.3))), 0.05, 0.3),
        "counts": draw_counts(jax.random.fold_in(key_list[7], 71), 0),
        "migration_plan": draw_migration_plan(jax.random.fold_in(key_list[7], 71), 0),
    }


REF_COUPLING = 0.7

def material_response(strain, plastic, bulk_modulus, shear_modulus, yield_radius):
    elastic = strain - plastic
    volumetric = elastic[..., 0, :, :, :] + elastic[..., 1, :, :, :] + elastic[..., 2, :, :, :]
    mean_normal = volumetric / 3.0
    deviator = jnp.stack([elastic[..., 0, :, :, :] - mean_normal, elastic[..., 1, :, :, :] - mean_normal, elastic[..., 2, :, :, :] - mean_normal, elastic[..., 3, :, :, :], elastic[..., 4, :, :, :], elastic[..., 5, :, :, :]], axis=-4)
    trial_deviator = 2.0 * shear_modulus * deviator
    weights = jnp.array([1.0, 1.0, 1.0, 2.0, 2.0, 2.0], jnp.float32).reshape(6, 1, 1, 1)
    squared = lax.optimization_barrier(jnp.sum(weights * trial_deviator * trial_deviator, axis=-4))
    factor = yield_radius / jnp.sqrt(jnp.maximum(squared, yield_radius * yield_radius))
    relaxed = factor[..., None, :, :, :] * trial_deviator
    normal_mask = jnp.array([1.0, 1.0, 1.0, 0.0, 0.0, 0.0], jnp.float32).reshape(6, 1, 1, 1)
    stress = relaxed + normal_mask * (bulk_modulus * volumetric)[..., None, :, :, :]
    increment = (trial_deviator - relaxed) / (2.0 * shear_modulus)
    return (stress, increment)

def green_apply(real_part, imag_part):
    extent = real_part.shape[-1]
    wavenumber = ((jnp.arange(extent) + extent // 2) % extent - extent // 2).astype(jnp.float32)
    freq_a = wavenumber[:, None, None]
    freq_b = wavenumber[None, :, None]
    freq_c = wavenumber[None, None, :]
    magnitude = freq_a * freq_a + freq_b * freq_b + freq_c * freq_c
    nonzero = magnitude > 0.0
    guarded = jnp.maximum(magnitude, 1.0)
    linear_term = jnp.where(nonzero, 1.0 / (2.0 * guarded), 0.0)
    cubic_term = jnp.where(nonzero, REF_COUPLING / (guarded * guarded), 0.0)

    def single(tau):
        tau_aa, tau_bb, tau_cc = (tau[:, 0], tau[:, 1], tau[:, 2])
        tau_bc, tau_ac, tau_ab = (tau[:, 3], tau[:, 4], tau[:, 5])
        traction_a = tau_aa * freq_a + tau_ab * freq_b + tau_ac * freq_c
        traction_b = tau_ab * freq_a + tau_bb * freq_b + tau_bc * freq_c
        traction_c = tau_ac * freq_a + tau_bc * freq_b + tau_cc * freq_c
        normal_part = freq_a * traction_a + freq_b * traction_b + freq_c * traction_c
        result_list = [linear_term * 2.0 * freq_a * traction_a - cubic_term * freq_a * freq_a * normal_part, linear_term * 2.0 * freq_b * traction_b - cubic_term * freq_b * freq_b * normal_part, linear_term * 2.0 * freq_c * traction_c - cubic_term * freq_c * freq_c * normal_part, linear_term * (freq_b * traction_c + freq_c * traction_b) - cubic_term * freq_b * freq_c * normal_part, linear_term * (freq_a * traction_c + freq_c * traction_a) - cubic_term * freq_a * freq_c * normal_part, linear_term * (freq_a * traction_b + freq_b * traction_a) - cubic_term * freq_a * freq_b * normal_part]
        return jnp.stack(result_list, axis=1)
    return (single(real_part), single(imag_part))

def polarization_update(stress):
    spectrum = jnp.fft.fftn(stress, axes=(-3, -2, -1))
    real_part, imag_part = green_apply(jnp.real(spectrum), jnp.imag(spectrum))
    return jnp.real(jnp.fft.ifftn(lax.complex(real_part, imag_part), axes=(-3, -2, -1)))

def element_strain(displacement):
    padded = jnp.pad(displacement, ((0, 0), (0, 1), (0, 1), (0, 1)))
    gradient = [[0.0, 0.0, 0.0], [0.0, 0.0, 0.0], [0.0, 0.0, 0.0]]
    for shift_a in (0, 1):
        for shift_b in (0, 1):
            for shift_c in (0, 1):
                corner_values = padded[:, shift_a:shift_a + NX, shift_b:shift_b + NY, shift_c:shift_c + NZ]
                signs = ((2 * shift_a - 1) / 4.0, (2 * shift_b - 1) / 4.0, (2 * shift_c - 1) / 4.0)
                for component in range(3):
                    for direction in range(3):
                        gradient[component][direction] = gradient[component][direction] + corner_values[component] * signs[direction]
    return jnp.stack([gradient[0][0], gradient[1][1], gradient[2][2], 0.5 * (gradient[1][2] + gradient[2][1]), 0.5 * (gradient[0][2] + gradient[2][0]), 0.5 * (gradient[0][1] + gradient[1][0])], axis=0)

def nodal_forces(stress_field):
    padded = jnp.pad(stress_field, ((0, 0), (1, 0), (1, 0), (1, 0)))
    pairs = [[0, 5, 4], [5, 1, 3], [4, 3, 2]]
    forces = [0.0, 0.0, 0.0]
    for shift_a in (0, 1):
        for shift_b in (0, 1):
            for shift_c in (0, 1):
                corner_values = padded[:, 1 - shift_a:1 - shift_a + NX, 1 - shift_b:1 - shift_b + NY, 1 - shift_c:1 - shift_c + NZ]
                signs = ((2 * shift_a - 1) / 4.0, (2 * shift_b - 1) / 4.0, (2 * shift_c - 1) / 4.0)
                for component in range(3):
                    for direction in range(3):
                        forces[component] = forces[component] + corner_values[pairs[component][direction]] * signs[direction]
    return jnp.stack(forces, axis=0)

def reference(displacement, plastic, bulk_modulus, shear_modulus, yield_radius, counts, migration_plan):
    strain_field = element_strain(displacement)
    strain_rows = strain_field.reshape(6, NE).T
    bulk_grid = bulk_modulus.reshape(G, G, G)
    shear_grid = shear_modulus.reshape(G, G, G)
    radius_grid = yield_radius.reshape(G, G, G)
    plastic_blocks = plastic.reshape(NE // RBLK, RBLK, 6, G, G, G)
    strain_blocks = strain_rows.reshape(NE // RBLK, RBLK, 6)
    count_blocks = counts.reshape(NE // RBLK, RBLK)

    def solve_block(inputs):
        plastic_block, strain_block, count_block = inputs
        strain = jnp.broadcast_to(strain_block[:, :, None, None, None], plastic_block.shape)
        previous_map = strain
        previous_update = jnp.zeros_like(strain)
        for step_index in range(ITER_PEAK):
            stress, unused = material_response(strain, plastic_block, bulk_grid, shear_grid, radius_grid)
            update = polarization_update(stress)
            mapped = strain - update
            change = update - previous_update
            numerator = lax.optimization_barrier(jnp.mean(change * update, axis=(1, 2, 3, 4)))
            denominator = lax.optimization_barrier(jnp.mean(change * change, axis=(1, 2, 3, 4))) + 1e-06
            weight = numerator / denominator if step_index > 0 else jnp.zeros_like(numerator)
            candidate = mapped - weight[:, None, None, None, None] * (mapped - previous_map)
            active = step_index < count_block
            strain = jnp.where(active[:, None, None, None, None], candidate, strain)
            previous_map = mapped
            previous_update = update
        stress, increment = material_response(strain, plastic_block, bulk_grid, shear_grid, radius_grid)
        return (lax.optimization_barrier(jnp.mean(stress, axis=(2, 3, 4))), plastic_block + increment)
    averages, updated = lax.map(solve_block, (plastic_blocks, strain_blocks, count_blocks))
    stress_field = averages.reshape(NE, 6).T.reshape(6, NX, NY, NZ)
    force = nodal_forces(stress_field)
    updated = updated.reshape(NE, 6, G, G * G)
    moved = jnp.zeros_like(updated).at[migration_plan].set(updated)
    return (force, moved)
```

```python
import math

import jax
import jax.numpy as jnp
import numpy as np
from jax import lax
from jax.experimental import pallas as pl
from jax.experimental.pallas import tpu as pltpu
from jax.sharding import PartitionSpec as P

COUPLING = 0.7
PAIRS = [(0, 0), (1, 1), (2, 2), (1, 2), (0, 2), (0, 1)]
SYM = [(m, n) for m in range(6) for n in range(m, 6)]


def symbol_table(extent):
    wave = ((np.arange(extent) + extent // 2) % extent - extent // 2).astype(np.float64)
    grid = np.meshgrid(wave, wave, wave, indexing="ij")
    square = grid[0] ** 2 + grid[1] ** 2 + grid[2] ** 2
    live = square > 0
    safe = np.where(live, square, 1.0)
    full = np.zeros((6, 6) + square.shape)
    for n, (p, q) in enumerate(PAIRS):
        traction = [np.zeros_like(square) for _ in range(3)]
        traction[p] = traction[p] + grid[q]
        if p != q:
            traction[q] = traction[q] + grid[p]
        normal = sum(grid[i] * traction[i] for i in range(3))
        weight = 1.0 if p == q else 2.0
        for m, (i, j) in enumerate(PAIRS):
            value = (grid[j] * traction[i] + grid[i] * traction[j]) / (2.0 * safe)
            value = value - COUPLING * grid[i] * grid[j] * normal / safe**2
            full[m, n] = np.where(live, value, 0.0) / weight
    flip = (-np.arange(extent)) % extent
    mirrored = full[:, :, flip][:, :, :, flip][:, :, :, :, flip]
    real = 0.5 * (full + mirrored) / extent**3
    half = extent // 2
    scale = np.where((np.arange(half + 1) % half) == 0, 1.0, 2.0).reshape(-1, 1)
    table = np.zeros((len(SYM), extent, extent * extent))
    for index, (m, n) in enumerate(SYM):
        table[index, : half + 1] = real[m, n, : half + 1].reshape(half + 1, -1) * scale
    return table.astype(np.float32)


def plane_tables(extent):
    plane = np.arange(extent * extent)
    row, col = plane // extent, plane % extent
    phase = (row[:, None] * row[None, :] + col[:, None] * col[None, :]) % extent
    angle = 2.0 * np.pi * phase / extent
    out = []
    for value in (np.cos(angle) + np.sin(angle), np.cos(angle) - np.sin(angle)):
        value = value.astype(np.float32)
        high = value.astype(jnp.bfloat16)
        low = (value - high.astype(np.float32)).astype(jnp.bfloat16)
        out.append(np.concatenate([high, high, low], axis=0))
    return np.stack(out)


C1, C2, C3 = math.cos(math.pi / 8), math.cos(math.pi / 4), math.cos(3 * math.pi / 8)


def cosine_sums(first, s, last):
    p = [s[j - 1] + s[7 - j] for j in (1, 2, 3)]
    m = [s[j - 1] - s[7 - j] for j in (1, 2, 3)]
    mid = s[3]
    total, diff = first + last, first - last
    t = m[1] * C2
    u, v = diff + t, diff - t
    w1 = m[0] * C1 + m[2] * C3
    w3 = m[0] * C3 - m[2] * C1
    plus, minus = total + mid, total - mid
    outer, inner = p[0] + p[2], (p[0] - p[2]) * C2
    even = plus + p[1]
    return [
        even + outer, u + w1, minus + inner, v + w3, plus - p[1],
        v - w3, minus - inner, u - w1, even - outer,
    ]


def sine_sums(d):
    n = [d[j - 1] + d[7 - j] for j in (1, 2, 3)]
    r = [d[j - 1] - d[7 - j] for j in (1, 2, 3)]
    mid = d[3]
    y1 = n[0] * C3 + n[2] * C1
    y3 = n[0] * C1 - n[2] * C3
    g = n[1] * C2
    gp, gm = g + mid, g - mid
    e = (r[0] + r[2]) * C2
    return [y1 + gp, e + r[1], y3 + gm, r[0] - r[2], y3 - gm, e - r[1], y1 - gp]


def split_dot(x, weights):
    high = x.astype(jnp.bfloat16)
    low = (x - high.astype(jnp.float32)).astype(jnp.bfloat16)
    stacked = jnp.concatenate([high, low, high], axis=1)
    return jnp.dot(stacked, weights, preferred_element_type=jnp.float32)


def elastic_parts(strain, plastic, shear2):
    elastic = [strain[c] - plastic[c] for c in range(6)]
    volume = elastic[0] + elastic[1] + elastic[2]
    mean = volume * (1.0 / 3.0)
    dev = [elastic[c] - mean for c in range(3)] + elastic[3:]
    normal = dev[0] * dev[0] + dev[1] * dev[1] + dev[2] * dev[2]
    shear = dev[3] * dev[3] + dev[4] * dev[4] + dev[5] * dev[5]
    size = (normal + (shear + shear)) * (shear2 * shear2)
    return volume, dev, size


def solve(extent, rows, state, out, strain_cols, count_col, top_count, mats, consts, scratch):
    bulk_ref, shear_ref, radius_ref = mats
    table_ref, plane_ref = consts
    pl_ref, e_ref, u_ref, a_ref, b_ref, a2_ref, b2_ref, t_ref = scratch
    half = extent // 2
    wide = extent * extent
    step = 6 * extent
    lanes = 128
    group = 6 * rows

    for c in range(6):
        column = jnp.broadcast_to(strain_cols[c], (rows, wide))
        for a in range(extent):
            for tile in range(wide // lanes):
                picked = state[tile, pl.ds(c * extent + a, rows, stride=step), :]
                pl_ref[c, a, :, pl.ds(tile * lanes, lanes)] = picked
            e_ref[c, a] = column
            u_ref[0, c, a] = jnp.zeros((rows, wide), jnp.float32)
            u_ref[1, c, a] = jnp.zeros((rows, wide), jnp.float32)

    def current(a, tile, k, alpha, beta):
        lane = pl.ds(tile * lanes, lanes)
        newer, older = (k + 1) & 1, k & 1
        values = []
        for c in range(6):
            v = e_ref[c, a, :, lane] - alpha * u_ref[newer, c, a, :, lane]
            values.append(v - beta * u_ref[older, c, a, :, lane])
        plastic = [pl_ref[c, a, :, lane] for c in range(6)]
        shear2 = 2.0 * shear_ref[pl.ds(a, 1), lane]
        radius = radius_ref[pl.ds(a, 1), lane]
        bulk = bulk_ref[pl.ds(a, 1), lane]
        volume, dev, size = elastic_parts(values, plastic, shear2)
        factor = radius * lax.rsqrt(jnp.maximum(size, radius * radius))
        gain = factor * shear2
        pressure = bulk * volume
        stress = [gain * dev[c] + pressure for c in range(3)]
        stress += [gain * dev[c] for c in range(3, 6)]
        return values, plastic, dev, factor, stress

    def sweep(k, carry):
        alpha, beta, before = carry
        for a in range(extent):
            for tile in range(wide // lanes):
                lane = pl.ds(tile * lanes, lanes)
                values, _, _, _, stress = current(a, tile, k, alpha, beta)
                for c in range(6):
                    e_ref[c, a, :, lane] = values[c]
                    t_ref[c, a, :, lane] = stress[c]
        for c in range(6):
            for tile in range(wide // lanes):
                lane = pl.ds(tile * lanes, lanes)
                x = [t_ref[c, a, :, lane] for a in range(extent)]
                s = [x[j] + x[extent - j] for j in range(1, half)]
                d = [x[j] - x[extent - j] for j in range(1, half)]
                for kk, value in enumerate(cosine_sums(x[0], s, x[half])):
                    a_ref[pl.ds(kk * group + c * rows, rows), lane] = value
                for kk, value in enumerate(sine_sums(d)):
                    b_ref[pl.ds(kk * group + c * rows, rows), lane] = value
        a2_ref[...] = split_dot(a_ref[...], plane_ref[0])
        b2_ref[...] = split_dot(b_ref[...], plane_ref[1])
        for kk in range(half + 1):
            ends = kk == 0 or kk == half
            for tile in range(wide // lanes):
                lane = pl.ds(tile * lanes, lanes)
                coef = {}
                for index, pair in enumerate(SYM):
                    coef[pair] = table_ref[index, pl.ds(kk, 1), lane]
                    coef[pair[::-1]] = coef[pair]

                def place(c, odd):
                    if ends:
                        return a2_ref, a_ref, pl.ds(kk * group + c * rows, rows)
                    if (c >= 4) != odd:
                        return b2_ref, b_ref, pl.ds((kk - 1) * group + c * rows, rows)
                    return a2_ref, a_ref, pl.ds(kk * group + c * rows, rows)

                for odd in (False,) if ends else (False, True):
                    tau = []
                    for c in range(6):
                        src, _, where = place(c, odd)
                        value = src[where, lane]
                        tau.append(value if c < 3 else value + value)
                    for m in range(6):
                        acc = coef[m, 0] * tau[0]
                        for n in range(1, 6):
                            acc = acc + coef[m, n] * tau[n]
                        _, dst, where = place(m, odd)
                        dst[where, lane] = acc
        a2_ref[...] = split_dot(a_ref[...], plane_ref[0])
        b2_ref[...] = split_dot(b_ref[...], plane_ref[1])
        num = jnp.zeros((rows, lanes), jnp.float32)
        den = jnp.zeros((rows, lanes), jnp.float32)
        newest, last = k & 1, (k + 1) & 1
        for c in range(6):
            for tile in range(wide // lanes):
                lane = pl.ds(tile * lanes, lanes)
                ca = [a2_ref[pl.ds(kk * group + c * rows, rows), lane] for kk in range(half + 1)]
                sb = [b2_ref[pl.ds(kk * group + c * rows, rows), lane] for kk in range(half - 1)]
                even = cosine_sums(ca[0], ca[1:half], ca[half])
                odd = [None] + sine_sums(sb)
                for a in range(extent):
                    j = min(a, extent - a)
                    if a == 0 or a == half:
                        value = even[j]
                    elif a < half:
                        value = even[j] + odd[j]
                    else:
                        value = even[j] - odd[j]
                    change = value - u_ref[last, c, a, :, lane]
                    num = num + change * value
                    den = den + change * change
                    u_ref[newest, c, a, :, lane] = value
        scale = 1.0 / (6 * extent**3)
        top = jnp.sum(num, axis=1, keepdims=True) * scale
        bottom = jnp.sum(den, axis=1, keepdims=True) * scale + 1e-06
        weight = jnp.where(k > 0, top / bottom, 0.0)
        active = jnp.where(count_col > k.astype(jnp.float32), 1.0, 0.0)
        alpha = active * (1.0 - weight)
        beta = active * weight * before
        spread = lambda v: jnp.broadcast_to(v, (rows, lanes))
        return spread(alpha), spread(beta), weight

    zero = jnp.zeros((rows, lanes), jnp.float32)
    alpha, beta, _ = lax.fori_loop(
        0, top_count, sweep, (zero, zero, jnp.zeros((rows, 1), jnp.float32))
    )
    sums = [jnp.zeros((rows, lanes), jnp.float32) for _ in range(6)]
    for a in range(extent):
        for tile in range(wide // lanes):
            lane = pl.ds(tile * lanes, lanes)
            _, plastic, dev, factor, stress = current(a, tile, top_count, alpha, beta)
            rest = 1.0 - factor
            for c in range(6):
                sums[c] = sums[c] + stress[c]
                where = pl.ds(c * extent + a, rows, stride=step)
                out[tile, where, :] = plastic[c] + rest * dev[c]
    return sums


def solve_scratch(extent, rows):
    half, wide = extent // 2, extent * extent
    field = (6, extent, rows, wide)
    f32 = jnp.float32
    return [
        pltpu.VMEM(field, f32),
        pltpu.VMEM(field, f32),
        pltpu.VMEM((2,) + field, f32),
        pltpu.VMEM(((half + 1) * 6 * rows, wide), f32),
        pltpu.VMEM(((half - 1) * 6 * rows, wide), f32),
        pltpu.VMEM(((half + 1) * 6 * rows, wide), f32),
        pltpu.VMEM(((half - 1) * 6 * rows, wide), f32),
        pltpu.VMEM(field, f32),
    ]


def to_column(row, mask):
    return jnp.sum(jnp.where(mask, jnp.broadcast_to(row, mask.shape), 0.0), axis=1, keepdims=True)


def to_row(column, mask):
    return jnp.sum(jnp.where(mask, jnp.broadcast_to(column, mask.shape), 0.0), axis=0, keepdims=True)


def row_copies(hbm_row, stage, row, sems, extent):
    lanes = 128
    step = 6 * extent
    pairs = []
    for tile in range(extent * extent // lanes):
        inside = stage.at[tile, pl.ds(row * step, step), :]
        pairs.append((hbm_row.at[:, pl.ds(tile * lanes, lanes)], inside, sems.at[row, tile]))
    return pairs


def counts_column(counts, rows):
    where = lax.broadcasted_iota(jnp.int32, (rows, 1), 0)
    column = jnp.zeros((rows, 1), jnp.float32)
    top = counts[0]
    for r in range(rows):
        column = jnp.where(where == r, counts[r].astype(jnp.float32), column)
        top = jnp.maximum(top, counts[r])
    return column, top


def lane_mask(rows):
    shape = (rows, 128)
    return lax.broadcasted_iota(jnp.int32, shape, 0) == lax.broadcasted_iota(jnp.int32, shape, 1)


def spread_nodes(value):
    return value, pltpu.roll(value, 127, 1)


def strain_rows(corners):
    pairs = [spread_nodes(v) for v in corners]
    total = [lo + hi for lo, hi in pairs]
    rise = [hi - lo for lo, hi in pairs]
    h = [
        0.25 * ((total[1] + total[3]) - (total[0] + total[2])),
        0.25 * ((total[2] + total[3]) - (total[0] + total[1])),
        0.25 * ((rise[0] + rise[1]) + (rise[2] + rise[3])),
    ]
    pick = lambda i, j: h[j][i : i + 1]
    return [
        pick(0, 0), pick(1, 1), pick(2, 2),
        0.5 * (pick(1, 2) + pick(2, 1)),
        0.5 * (pick(0, 2) + pick(2, 0)),
        0.5 * (pick(0, 1) + pick(1, 0)),
    ]


def force_kernel(own, low_a, low_b, low_ab, out):
    total, rise = [], []
    for ref in (own, low_a, low_b, low_ab):
        value = ref[...]
        below = pltpu.roll(value, 1, 1)
        total.append(value + below)
        rise.append(below - value)
    along = [
        (total[1] + total[3]) - (total[0] + total[2]),
        (total[2] + total[3]) - (total[0] + total[1]),
        (rise[0] + rise[1]) + (rise[2] + rise[3]),
    ]
    index = [[0, 5, 4], [5, 1, 3], [4, 3, 2]]
    for i in range(3):
        parts = [along[j][index[i][j] : index[i][j] + 1] for j in range(3)]
        out[i : i + 1] = 0.25 * (parts[0] + parts[1] + parts[2])


def source_kernel(extent, rows, *refs):
    (d0, d1, d2, d3, counts, plastic, bulk, shear, radius, table, plane) = refs[:11]
    next_out, averages = refs[11:13]
    stage, result, sems = refs[13:16]
    scratch = refs[16:]
    loads = []
    for r in range(rows):
        for src, dst, sem in row_copies(plastic.at[r], stage, r, sems.at[0], extent):
            loads.append(pltpu.make_async_copy(src, dst, sem))
    for copy in loads:
        copy.start()
    mask = lane_mask(rows)
    strain = [to_column(v, mask) for v in strain_rows([d0[...], d1[...], d2[...], d3[...]])]
    column, top = counts_column(counts, rows)
    for copy in loads:
        copy.wait()
    sums = solve(
        extent, rows, stage, result, strain, column, top,
        (bulk, shear, radius), (table, plane), scratch,
    )
    stores = []
    for r in range(rows):
        for dst, src, sem in row_copies(next_out.at[r], result, r, sems.at[1], extent):
            stores.append(pltpu.make_async_copy(src, dst, sem))
    for copy in stores:
        copy.start()
    averages[...] = jnp.zeros(averages.shape, jnp.float32)
    for c in range(6):
        mean = jnp.sum(sums[c], axis=1, keepdims=True) * (1.0 / extent**3)
        averages[c : c + 1] = to_row(mean, mask)
    for copy in stores:
        copy.wait()


def shift_pairs(counts, steps):
    pairs = []
    for flat in range(math.prod(counts)):
        at, rest = [], flat
        for size in reversed(counts):
            at.insert(0, rest % size)
            rest //= size
        to = [p + s for p, s in zip(at, steps)]
        if all(0 <= t < size for t, size in zip(to, counts)):
            target = 0
            for t, size in zip(to, counts):
                target = target * size + t
            pairs.append((flat, target))
    return pairs


def halo(value, step):
    layers = lax.axis_size("rve")
    columns = lax.axis_size("mic") * lax.axis_size("mac")
    everyone = ("rve", "mic", "mac")
    return (
        lax.ppermute(value, "rve", shift_pairs([layers], [step])),
        lax.ppermute(value, ("mic", "mac"), shift_pairs([columns], [step])),
        lax.ppermute(value, everyone, shift_pairs([layers, columns], [step, step])),
    )


def route_slots(migration_plan, width_rows, capacity):
    columns = lax.axis_size("mic") * lax.axis_size("mac")
    partner = migration_plan // width_rows // columns
    target_row = migration_plan % width_rows
    shared = partner[:, None] == partner[None, :]
    positions = jnp.arange(width_rows)
    earlier = positions[:, None] > positions[None, :]
    order_within = jnp.sum((shared & earlier).astype(jnp.int32), axis=1)
    return (partner * capacity + order_within, target_row)


def move_any(rows_next, migration_plan):
    width_rows = rows_next.shape[0]
    devices_along = lax.axis_size("rve")
    peers_used = min(devices_along // 2, width_rows // 2)
    capacity = width_rows // peers_used
    total = devices_along * capacity
    slot_index, target_row = route_slots(migration_plan, width_rows, capacity)
    matches = slot_index[None, :] == jnp.arange(total)[:, None]
    source = jnp.sum(jnp.where(matches, jnp.arange(width_rows)[None, :], 0), axis=1)
    labels = jnp.sum(jnp.where(matches, target_row[None, :] + 1, 0), axis=1)
    outgoing = jnp.take(rows_next, source, axis=0)
    arrived = lax.all_to_all(outgoing, "rve", split_axis=0, concat_axis=0, tiled=True)
    tags = lax.all_to_all(labels, "rve", split_axis=0, concat_axis=0, tiled=True)
    wanted = tags[None, :] == jnp.arange(1, width_rows + 1)[:, None]
    place = jnp.sum(jnp.where(wanted, jnp.arange(total)[None, :], 0), axis=1)
    return jnp.take(arrived, place, axis=0)


def on_device(displacement, plastic, bulk, shear, radius, counts, migration_plan):
    rows, _, extent, wide = plastic.shape
    depth = displacement.shape[3]
    f32 = jnp.float32
    table = jnp.asarray(symbol_table(extent))
    plane = jnp.asarray(plane_tables(extent))
    vmem = pl.BlockSpec(memory_space=pltpu.VMEM)
    smem = pl.BlockSpec(memory_space=pltpu.SMEM)
    anywhere = pl.BlockSpec(memory_space=pl.ANY)
    nodes = jnp.pad(displacement.reshape(3, depth), ((0, 0), (0, 128 - depth)))
    corners = (nodes,) + halo(nodes, -1)
    staging = [
        pltpu.VMEM((wide // 128, rows * 6 * extent, 128), f32),
        pltpu.VMEM((wide // 128, rows * 6 * extent, 128), f32),
        pltpu.SemaphoreType.DMA((2, rows, wide // 128)),
    ]
    finished, averages = pl.pallas_call(
        lambda *refs: source_kernel(extent, rows, *refs),
        out_shape=(
            jax.ShapeDtypeStruct((rows, 6 * extent, wide), f32),
            jax.ShapeDtypeStruct((8, 128), f32),
        ),
        in_specs=[vmem] * 4 + [smem, anywhere] + [vmem] * 5,
        out_specs=(anywhere, vmem),
        scratch_shapes=staging + solve_scratch(extent, rows),
        compiler_params=pltpu.CompilerParams(vmem_limit_bytes=56 * 2**20),
        name="solve_source",
    )(*corners, counts, plastic.reshape(rows, 6 * extent, wide), bulk, shear, radius, table, plane)
    sides = (averages,) + halo(averages, 1)
    force = pl.pallas_call(
        force_kernel,
        out_shape=jax.ShapeDtypeStruct((3, 128), f32),
        in_specs=[vmem] * 4,
        out_specs=vmem,
        name="force",
    )(*sides)
    force = force[:, :depth].reshape(displacement.shape)
    return force, move_any(finished, migration_plan).reshape(plastic.shape)


def solution(mesh):
    everyone = ("rve", "mic", "mac")
    return jax.shard_map(
        on_device,
        mesh=mesh,
        in_specs=(
            P(None, "rve", ("mic", "mac"), None),
            P(everyone, None, None, None),
            P(), P(), P(),
            P(everyone),
            P(everyone),
        ),
        out_specs=(P(None, "rve", ("mic", "mac"), None), P(everyone, None, None, None)),
        check_vma=False,
    )
```

```python
import math

import jax
import jax.numpy as jnp
import numpy as np
from jax import lax
from jax.experimental import pallas as pl
from jax.experimental.pallas import tpu as pltpu
from jax.sharding import PartitionSpec as P


COUPLING = 0.7
EARLY = 2
VMEM_BYTES = 48 * 2**20
PAIRS = [(0, 0), (1, 1), (2, 2), (1, 2), (0, 2), (0, 1)]
SYM = [(m, n) for m in range(6) for n in range(m, 6)]


def symbol_table(extent):
    wave = ((np.arange(extent) + extent // 2) % extent - extent // 2).astype(np.float64)
    grid = np.meshgrid(wave, wave, wave, indexing="ij")
    square = grid[0] ** 2 + grid[1] ** 2 + grid[2] ** 2
    live = square > 0
    safe = np.where(live, square, 1.0)
    full = np.zeros((6, 6) + square.shape)
    for n, (p, q) in enumerate(PAIRS):
        traction = [np.zeros_like(square) for _ in range(3)]
        traction[p] = traction[p] + grid[q]
        if p != q:
            traction[q] = traction[q] + grid[p]
        normal = sum(grid[i] * traction[i] for i in range(3))
        weight = 1.0 if p == q else 2.0
        for m, (i, j) in enumerate(PAIRS):
            value = (grid[j] * traction[i] + grid[i] * traction[j]) / (2.0 * safe)
            value = value - COUPLING * grid[i] * grid[j] * normal / safe**2
            full[m, n] = np.where(live, value, 0.0) / weight
    flip = (-np.arange(extent)) % extent
    mirrored = full[:, :, flip][:, :, :, flip][:, :, :, :, flip]
    real = 0.5 * (full + mirrored) / extent**3
    half = extent // 2
    scale = np.where((np.arange(half + 1) % half) == 0, 1.0, 2.0).reshape(-1, 1)
    table = np.zeros((len(SYM), extent, extent * extent))
    for index, (m, n) in enumerate(SYM):
        table[index, : half + 1] = real[m, n, : half + 1].reshape(half + 1, -1) * scale
    return table.astype(np.float32)


def plane_tables(extent):
    plane = np.arange(extent * extent)
    row, col = plane // extent, plane % extent
    phase = (row[:, None] * row[None, :] + col[:, None] * col[None, :]) % extent
    angle = 2.0 * np.pi * phase / extent
    out = []
    for value in (np.cos(angle) + np.sin(angle), np.cos(angle) - np.sin(angle)):
        value = value.astype(np.float32)
        high = value.astype(jnp.bfloat16)
        low = (value - high.astype(np.float32)).astype(jnp.bfloat16)
        out.append(np.concatenate([high, high, low], axis=0))
    return np.stack(out)


C1, C2, C3 = math.cos(math.pi / 8), math.cos(math.pi / 4), math.cos(3 * math.pi / 8)


def cosine_sums(first, s, last):
    p = [s[j - 1] + s[7 - j] for j in (1, 2, 3)]
    m = [s[j - 1] - s[7 - j] for j in (1, 2, 3)]
    mid = s[3]
    total, diff = first + last, first - last
    t = m[1] * C2
    u, v = diff + t, diff - t
    w1 = m[0] * C1 + m[2] * C3
    w3 = m[0] * C3 - m[2] * C1
    plus, minus = total + mid, total - mid
    outer, inner = p[0] + p[2], (p[0] - p[2]) * C2
    even = plus + p[1]
    return [
        even + outer, u + w1, minus + inner, v + w3, plus - p[1],
        v - w3, minus - inner, u - w1, even - outer,
    ]


def sine_sums(d):
    n = [d[j - 1] + d[7 - j] for j in (1, 2, 3)]
    r = [d[j - 1] - d[7 - j] for j in (1, 2, 3)]
    mid = d[3]
    y1 = n[0] * C3 + n[2] * C1
    y3 = n[0] * C1 - n[2] * C3
    g = n[1] * C2
    gp, gm = g + mid, g - mid
    e = (r[0] + r[2]) * C2
    return [y1 + gp, e + r[1], y3 + gm, r[0] - r[2], y3 - gm, e - r[1], y1 - gp]


def split_dot(x, weights):
    high = x.astype(jnp.bfloat16)
    low = (x - high.astype(jnp.float32)).astype(jnp.bfloat16)
    stacked = jnp.concatenate([high, low, high], axis=1)
    return jnp.dot(stacked, weights, preferred_element_type=jnp.float32)


def elastic_parts(strain, plastic, shear2):
    elastic = [strain[c] - plastic[c] for c in range(6)]
    volume = elastic[0] + elastic[1] + elastic[2]
    mean = volume * (1.0 / 3.0)
    dev = [elastic[c] - mean for c in range(3)] + elastic[3:]
    normal = dev[0] * dev[0] + dev[1] * dev[1] + dev[2] * dev[2]
    shear = dev[3] * dev[3] + dev[4] * dev[4] + dev[5] * dev[5]
    size = (normal + (shear + shear)) * (shear2 * shear2)
    return volume, dev, size


def solve(extent, rows, state, out, strain_cols, late_counts, mats, consts, scratch):
    bulk_ref, shear_ref, radius_ref = mats
    table_ref, plane_ref = consts
    pl_ref, e_ref, u_ref, a_ref, b_ref, a2_ref, b2_ref, t_ref = scratch
    half = extent // 2
    wide = extent * extent
    step = 6 * extent
    lanes = 128
    group = 6 * rows

    for c in range(6):
        column = jnp.broadcast_to(strain_cols[c], (rows, wide))
        for a in range(extent):
            for tile in range(wide // lanes):
                picked = state[tile, pl.ds(c * extent + a, rows, stride=step), :]
                pl_ref[c, a, :, pl.ds(tile * lanes, lanes)] = picked
            e_ref[c, a] = column
            u_ref[0, c, a] = jnp.zeros((rows, wide), jnp.float32)
            u_ref[1, c, a] = jnp.zeros((rows, wide), jnp.float32)
    count_col, top_count = late_counts()

    def current(a, tile, k, alpha, beta):
        lane = pl.ds(tile * lanes, lanes)
        newer, older = (k + 1) & 1, k & 1
        values = []
        for c in range(6):
            v = e_ref[c, a, :, lane] - alpha * u_ref[newer, c, a, :, lane]
            values.append(v - beta * u_ref[older, c, a, :, lane])
        plastic = [pl_ref[c, a, :, lane] for c in range(6)]
        shear2 = 2.0 * shear_ref[pl.ds(a, 1), lane]
        radius = radius_ref[pl.ds(a, 1), lane]
        bulk = bulk_ref[pl.ds(a, 1), lane]
        volume, dev, size = elastic_parts(values, plastic, shear2)
        factor = radius * lax.rsqrt(jnp.maximum(size, radius * radius))
        gain = factor * shear2
        pressure = bulk * volume
        stress = [gain * dev[c] + pressure for c in range(3)]
        stress += [gain * dev[c] for c in range(3, 6)]
        return values, plastic, dev, factor, stress

    def sweep(k, carry):
        alpha, beta, before = carry
        for a in range(extent):
            for tile in range(wide // lanes):
                lane = pl.ds(tile * lanes, lanes)
                values, _, _, _, stress = current(a, tile, k, alpha, beta)
                for c in range(6):
                    e_ref[c, a, :, lane] = values[c]
                    t_ref[c, a, :, lane] = stress[c]
        for c in range(6):
            for tile in range(wide // lanes):
                lane = pl.ds(tile * lanes, lanes)
                x = [t_ref[c, a, :, lane] for a in range(extent)]
                s = [x[j] + x[extent - j] for j in range(1, half)]
                d = [x[j] - x[extent - j] for j in range(1, half)]
                for kk, value in enumerate(cosine_sums(x[0], s, x[half])):
                    a_ref[pl.ds(kk * group + c * rows, rows), lane] = value
                for kk, value in enumerate(sine_sums(d)):
                    b_ref[pl.ds(kk * group + c * rows, rows), lane] = value
        a2_ref[...] = split_dot(a_ref[...], plane_ref[0])
        b2_ref[...] = split_dot(b_ref[...], plane_ref[1])
        for kk in range(half + 1):
            ends = kk == 0 or kk == half
            for tile in range(wide // lanes):
                lane = pl.ds(tile * lanes, lanes)
                coef = {}
                for index, pair in enumerate(SYM):
                    coef[pair] = table_ref[index, pl.ds(kk, 1), lane]
                    coef[pair[::-1]] = coef[pair]

                def place(c, odd):
                    if ends:
                        return a2_ref, a_ref, pl.ds(kk * group + c * rows, rows)
                    if (c >= 4) != odd:
                        return b2_ref, b_ref, pl.ds((kk - 1) * group + c * rows, rows)
                    return a2_ref, a_ref, pl.ds(kk * group + c * rows, rows)

                for odd in (False,) if ends else (False, True):
                    tau = []
                    for c in range(6):
                        src, _, where = place(c, odd)
                        value = src[where, lane]
                        tau.append(value if c < 3 else value + value)
                    for m in range(6):
                        acc = coef[m, 0] * tau[0]
                        for n in range(1, 6):
                            acc = acc + coef[m, n] * tau[n]
                        _, dst, where = place(m, odd)
                        dst[where, lane] = acc
        a2_ref[...] = split_dot(a_ref[...], plane_ref[0])
        b2_ref[...] = split_dot(b_ref[...], plane_ref[1])
        num = jnp.zeros((rows, lanes), jnp.float32)
        den = jnp.zeros((rows, lanes), jnp.float32)
        newest, last = k & 1, (k + 1) & 1
        for c in range(6):
            for tile in range(wide // lanes):
                lane = pl.ds(tile * lanes, lanes)
                ca = [a2_ref[pl.ds(kk * group + c * rows, rows), lane] for kk in range(half + 1)]
                sb = [b2_ref[pl.ds(kk * group + c * rows, rows), lane] for kk in range(half - 1)]
                even = cosine_sums(ca[0], ca[1:half], ca[half])
                odd = [None] + sine_sums(sb)
                for a in range(extent):
                    j = min(a, extent - a)
                    if a == 0 or a == half:
                        value = even[j]
                    elif a < half:
                        value = even[j] + odd[j]
                    else:
                        value = even[j] - odd[j]
                    change = value - u_ref[last, c, a, :, lane]
                    num = num + change * value
                    den = den + change * change
                    u_ref[newest, c, a, :, lane] = value
        scale = 1.0 / (6 * extent**3)
        top = jnp.sum(num, axis=1, keepdims=True) * scale
        bottom = jnp.sum(den, axis=1, keepdims=True) * scale + 1e-06
        weight = jnp.where(k > 0, top / bottom, 0.0)
        active = jnp.where(count_col > k.astype(jnp.float32), 1.0, 0.0)
        alpha = active * (1.0 - weight)
        beta = active * weight * before
        spread = lambda v: jnp.broadcast_to(v, (rows, lanes))
        return spread(alpha), spread(beta), weight

    zero = jnp.zeros((rows, lanes), jnp.float32)
    alpha, beta, _ = lax.fori_loop(
        0, top_count, sweep, (zero, zero, jnp.zeros((rows, 1), jnp.float32))
    )
    sums = [jnp.zeros((rows, lanes), jnp.float32) for _ in range(6)]
    for a in range(extent):
        for tile in range(wide // lanes):
            lane = pl.ds(tile * lanes, lanes)
            _, plastic, dev, factor, stress = current(a, tile, top_count, alpha, beta)
            rest = 1.0 - factor
            for c in range(6):
                sums[c] = sums[c] + stress[c]
                where = pl.ds(c * extent + a, rows, stride=step)
                out[tile, where, :] = plastic[c] + rest * dev[c]
    return sums


def solve_scratch(extent, rows):
    half, wide = extent // 2, extent * extent
    field = (6, extent, rows, wide)
    f32 = jnp.float32
    return [
        pltpu.VMEM(field, f32),
        pltpu.VMEM(field, f32),
        pltpu.VMEM((2,) + field, f32),
        pltpu.VMEM(((half + 1) * 6 * rows, wide), f32),
        pltpu.VMEM(((half - 1) * 6 * rows, wide), f32),
        pltpu.VMEM(((half + 1) * 6 * rows, wide), f32),
        pltpu.VMEM(((half - 1) * 6 * rows, wide), f32),
        pltpu.VMEM(field, f32),
    ]


def to_column(row, mask):
    return jnp.sum(jnp.where(mask, jnp.broadcast_to(row, mask.shape), 0.0), axis=1, keepdims=True)


def to_row(column, mask):
    return jnp.sum(jnp.where(mask, jnp.broadcast_to(column, mask.shape), 0.0), axis=0, keepdims=True)


def row_copies(hbm_row, stage, row, sems, extent):
    lanes = 128
    step = 6 * extent
    pairs = []
    for tile in range(extent * extent // lanes):
        inside = stage.at[tile, pl.ds(row * step, step), :]
        pairs.append((hbm_row.at[:, pl.ds(tile * lanes, lanes)], inside, sems.at[row, tile]))
    return pairs


def counts_column(counts, rows):
    where = lax.broadcasted_iota(jnp.int32, (rows, 1), 0)
    column = jnp.zeros((rows, 1), jnp.float32)
    top = counts[0]
    for r in range(rows):
        column = jnp.where(where == r, counts[r].astype(jnp.float32), column)
        top = jnp.maximum(top, counts[r])
    return column, top


def lane_mask(rows):
    shape = (rows, 128)
    return lax.broadcasted_iota(jnp.int32, shape, 0) == lax.broadcasted_iota(jnp.int32, shape, 1)


def spread_nodes(value):
    return value, pltpu.roll(value, 127, 1)


def strain_rows(corners):
    pairs = [spread_nodes(v) for v in corners]
    total = [lo + hi for lo, hi in pairs]
    rise = [hi - lo for lo, hi in pairs]
    h = [
        0.25 * ((total[1] + total[3]) - (total[0] + total[2])),
        0.25 * ((total[2] + total[3]) - (total[0] + total[1])),
        0.25 * ((rise[0] + rise[1]) + (rise[2] + rise[3])),
    ]
    pick = lambda i, j: h[j][i : i + 1]
    return [
        pick(0, 0), pick(1, 1), pick(2, 2),
        0.5 * (pick(1, 2) + pick(2, 1)),
        0.5 * (pick(0, 2) + pick(2, 0)),
        0.5 * (pick(0, 1) + pick(1, 0)),
    ]


def zero_below(value):
    return value, pltpu.roll(value, 1, 1)


def node_force(own, low_a, low_b, low_ab):
    total, rise = [], []
    for value in (own, low_a, low_b, low_ab):
        value, below = zero_below(value)
        total.append(value + below)
        rise.append(below - value)
    along = [
        (total[1] + total[3]) - (total[0] + total[2]),
        (total[2] + total[3]) - (total[0] + total[1]),
        (rise[0] + rise[1]) + (rise[2] + rise[3]),
    ]
    index = [[0, 5, 4], [5, 1, 3], [4, 3, 2]]
    rows = []
    for i in range(3):
        parts = [along[j][index[i][j] : index[i][j] + 1] for j in range(3)]
        rows.append(0.25 * (parts[0] + parts[1] + parts[2]))
    return rows


class Layout:
    def __init__(self, plastic_shape, depth, layers, columns):
        self.rows, _, self.extent, self.wide = plastic_shape
        self.depth, self.layers, self.columns = depth, layers, columns
        self.peers = min(layers // 2, self.rows // 2)
        self.capacity = self.rows // self.peers
        self.near = [k for k in (1, 2) if k < layers]
        self.early = (self.capacity * EARLY) // 4
        self.late = self.capacity - self.early
        self.step = 6 * self.extent
        self.meta = -(-self.capacity // 8) * 8

    def route(self, plan):
        here = lax.axis_index("rve")
        block = self.rows * self.columns
        partner = [lax.div(plan[e], block) for e in range(self.rows)]
        away = []
        for p in partner:
            d = p - here
            away.append(jnp.where(d < 0, d + self.layers, d))
        order = []
        for e in range(self.rows):
            before = jnp.int32(0)
            for f in range(e):
                before = before + (away[f] == away[e]).astype(jnp.int32)
            order.append(before)
        target = [lax.rem(plan[e], self.rows) for e in range(self.rows)]
        return away, order, target

    def pick(self, away, order, offset, place):
        row, found = jnp.int32(0), jnp.int32(0)
        for e in range(self.rows):
            hit = jnp.logical_and(away[e] == offset, order[e] == place)
            row = jnp.where(hit, e, row)
            found = jnp.where(hit, 1, found)
        return row, found


def pack_kernel(lay, *refs):
    displacement, plan, plastic = refs[:3]
    fixed = refs[3:8]
    nodes, state = refs[8:10]
    copied = refs[10:15]
    boxes = refs[15 : 15 + len(lay.near)]
    plan_s, corner, small_sems, box_sems, fix_sems, row_sems = refs[15 + len(lay.near) :]
    load_plan = pltpu.make_async_copy(plan, plan_s, small_sems.at[0])
    load_plan.start()
    load_corner = pltpu.make_async_copy(displacement, corner, small_sems.at[1])
    load_corner.start()
    copies = []
    for r in range(lay.rows):
        for src, dst, sem in row_copies(plastic.at[r], state, r, row_sems, lay.extent):
            copies.append(pltpu.make_async_copy(src, dst, sem))
    for i in range(len(fixed)):
        copies.append(pltpu.make_async_copy(fixed[i], copied[i], fix_sems.at[i]))
    for copy in copies:
        copy.start()
    nodes[...] = jnp.zeros(nodes.shape, jnp.float32)
    load_plan.wait()
    away, order, _ = lay.route(plan_s)
    packed = []
    for i, offset in enumerate(lay.near):
        for s in range(lay.early):
            row, _ = lay.pick(away, order, offset, s)
            packed.append(pltpu.make_async_copy(plastic.at[row], boxes[i].at[s], box_sems.at[i, s]))
            packed[-1].start()
    load_corner.wait()
    for i in range(3):
        nodes[i : i + 1, : lay.depth] = corner[i, 0]
    rare = jnp.int32(0)
    for e in range(lay.rows):
        usual = away[e] == 0
        for offset in lay.near:
            usual = jnp.logical_or(usual, away[e] == offset)
        rare = jnp.where(usual, rare, 1)
    nodes[3:4] = jnp.full((1, 128), rare.astype(jnp.float32))
    for copy in copies + packed:
        copy.wait()


def source_kernel(lay, *refs):
    extent, rows = lay.extent, lay.rows
    own, upper, side, counts, plan, state, bulk, shear, radius, table, plane = refs[:11]
    n = len(lay.near)
    finished, first = refs[11:13]
    others = refs[13 : 12 + n]
    at = 12 + max(n, 1)
    boxes = refs[at : at + n]
    counts_s, plan_s, small_sems, box_sems = refs[at + n : at + n + 4]
    scratch = refs[at + n + 4 :]
    small = [
        pltpu.make_async_copy(counts, counts_s, small_sems.at[0]),
        pltpu.make_async_copy(plan, plan_s, small_sems.at[1]),
    ]
    for copy in small:
        copy.start()
    mask = lane_mask(rows)
    inside = jnp.where(lax.axis_index("rve") < lay.layers - 1, 1.0, 0.0)
    corners = [own[0:3], upper[0:3] * inside, side[0:3], side[8:11] * inside]
    strain = [to_column(v, mask) for v in strain_rows(corners)]
    column = []

    def late_counts():
        for copy in small:
            copy.wait()
        values, top = counts_column(counts_s, rows)
        column.append(values)
        return values, top

    sums = solve(
        extent, rows, state, finished, strain, late_counts,
        (bulk, shear, radius), (table, plane), scratch,
    )
    away, order, target = lay.route(plan_s)
    stores = []
    for i, offset in enumerate(lay.near):
        for s in range(lay.late):
            row, _ = lay.pick(away, order, offset, lay.early + s)
            for tile in range(lay.wide // 128):
                start = pl.multiple_of(row * lay.step, 8)
                src = finished.at[tile, pl.ds(start, lay.step), :]
                dst = boxes[i].at[s, :, pl.ds(tile * 128, 128)]
                stores.append(pltpu.make_async_copy(src, dst, box_sems.at[i, s, tile]))
                stores[-1].start()
    lane = lax.broadcasted_iota(jnp.int32, (rows, 128), 1)
    sub = lax.broadcasted_iota(jnp.int32, (rows, 128), 0)
    card = jnp.zeros((rows, 128), jnp.float32)
    for c in range(6):
        card = jnp.where(lane == c, strain[c], card)
    card = jnp.where(lane == 6, column[0], card)
    for r in range(rows):
        label = (target[r] + 1).astype(jnp.float32)
        card = jnp.where(jnp.logical_and(lane == 7, sub == r), label, card)
    notes = (first,) + tuple(others)
    first[...] = jnp.zeros(first.shape, jnp.float32)
    for i, offset in enumerate(lay.near):
        base = 8 if i == 0 else 0
        if i:
            notes[i][...] = jnp.zeros(notes[i].shape, jnp.float32)
        for s in range(lay.capacity):
            row, found = lay.pick(away, order, offset, s)
            chosen = jnp.logical_and(sub == row, found > 0)
            line = jnp.sum(jnp.where(chosen, card, 0.0), axis=0, keepdims=True)
            line = jnp.where(lane[0:1] == 8, jnp.maximum(own[3:4], upper[3:4]), line)
            notes[i][base + s : base + s + 1] = line
    for c in range(6):
        mean = jnp.sum(sums[c], axis=1, keepdims=True) * (1.0 / extent**3)
        first[c : c + 1] = to_row(mean, mask)
    for copy in stores:
        copy.wait()


def note_row(i, s):
    return (8 if i == 0 else 0) + s


def target_kernel(lay, *refs):
    extent, rows, n = lay.extent, lay.rows, len(lay.near)
    notes, boxes = refs[:n], refs[n : 2 * n]
    own, upper, bulk, shear, radius, table, plane = refs[2 * n : 2 * n + 7]
    arrived, rare_out = refs[2 * n + 7 : 2 * n + 9]
    rest = refs[2 * n + 9 :]
    marks, rest = rest[:n], rest[n:]
    stage, result, load_sems, store_sems, mark_sems, cards = rest[:6]
    scratch = rest[6:]
    slots = [(i, s) for i in range(n) for s in range(lay.early)]
    reads = [pltpu.make_async_copy(notes[i], marks[i], mark_sems.at[i]) for i in range(n)]
    loads = []
    for r, (i, s) in enumerate(slots):
        for src, dst, sem in row_copies(boxes[i].at[s], stage, r, load_sems, extent):
            loads.append(pltpu.make_async_copy(src, dst, sem))
    for copy in reads + loads:
        copy.start()
    cards[...] = jnp.zeros(cards.shape, jnp.float32)
    for r, (i, s) in enumerate(slots):
        cards[r : r + 1] = notes[i][note_row(i, s) : note_row(i, s) + 1]
    card = cards[...]
    strain = [card[:, c : c + 1] for c in range(6)]

    def late_counts():
        for copy in reads:
            copy.wait()
        most = jnp.float32(0.0)
        for i, s in slots:
            most = jnp.maximum(most, marks[i][note_row(i, s), 6])
        return card[:, 6:7], most.astype(jnp.int32)

    rare = jnp.maximum(own[3:4], upper[3:4])
    for i in range(n):
        flag = notes[i][note_row(i, 0) : note_row(i, 0) + 1]
        rare = jnp.maximum(rare, jnp.broadcast_to(flag[:, 8:9], rare.shape))
    rare_out[...] = jnp.broadcast_to(rare, rare_out.shape)
    for copy in loads:
        copy.wait()
    solve(
        extent, rows, stage, result, strain, late_counts,
        (bulk, shear, radius), (table, plane), scratch,
    )
    moves = []
    for r, (i, s) in enumerate(slots):
        label = marks[i][note_row(i, s), 7].astype(jnp.int32)
        moves.append((r, label > 0, jnp.maximum(label - 1, 0)))
    for phase in ("start", "wait"):
        for r, valid, where in moves:

            @pl.when(valid)
            def _(r=r, where=where, phase=phase):
                for dst, src, sem in row_copies(arrived.at[where], result, r, store_sems, extent):
                    getattr(pltpu.make_async_copy(src, dst, sem), phase)()


def place_kernel(lay, *refs):
    n = len(lay.near)
    notes, boxes = refs[:n], refs[n : 2 * n]
    plan, finished, _, out = refs[2 * n : 2 * n + 4]
    marks, rest = refs[2 * n + 4 : 3 * n + 4], refs[3 * n + 4 :]
    plan_s, mark_sems, box_sems, row_sems = rest
    reads = [pltpu.make_async_copy(notes[i], marks[i], mark_sems.at[i]) for i in range(n)]
    reads.append(pltpu.make_async_copy(plan, plan_s, mark_sems.at[n]))
    for copy in reads:
        copy.start()
    for copy in reads:
        copy.wait()
    away, _, target = lay.route(plan_s)
    moves = []
    for i in range(n):
        for s in range(lay.late):
            label = marks[i][note_row(i, lay.early + s), 7].astype(jnp.int32)
            where = jnp.maximum(label - 1, 0)
            moves.append((label > 0, [(boxes[i].at[s], out.at[where], box_sems.at[i, s])]))
    for e in range(lay.rows):
        pieces = row_copies(out.at[target[e]], finished, e, row_sems, lay.extent)
        moves.append((away[e] == 0, [(src, dst, sem) for dst, src, sem in pieces]))
    for phase in ("start", "wait"):
        for valid, pieces in moves:

            @pl.when(valid)
            def _(pieces=pieces, phase=phase):
                for src, dst, sem in pieces:
                    getattr(pltpu.make_async_copy(src, dst, sem), phase)()


def force_kernel(lay, own, below, side, out):
    inside = jnp.where(lax.axis_index("rve") > 0, 1.0, 0.0)
    rows = node_force(own[0:6], below[0:6] * inside, side[0:6], side[8:14] * inside)
    for i in range(3):
        out[i, 0] = rows[i][:, : lay.depth]


def shift_pairs(counts, steps):
    pairs = []
    for flat in range(math.prod(counts)):
        at, rest = [], flat
        for size in reversed(counts):
            at.insert(0, rest % size)
            rest //= size
        to = [p + s for p, s in zip(at, steps)]
        if all(0 <= t < size for t, size in zip(to, counts)):
            target = 0
            for t, size in zip(to, counts):
                target = target * size + t
            pairs.append((flat, target))
    return pairs


def ring(value, step):
    layers = lax.axis_size("rve")
    return lax.ppermute(value, "rve", [(i, (i + step) % layers) for i in range(layers)])


def sideways(value, step):
    columns = lax.axis_size("mic") * lax.axis_size("mac")
    return lax.ppermute(value, ("mic", "mac"), shift_pairs([columns], [step]))


def route_slots(migration_plan, width_rows, capacity):
    columns = lax.axis_size("mic") * lax.axis_size("mac")
    partner = migration_plan // width_rows // columns
    target_row = migration_plan % width_rows
    shared = partner[:, None] == partner[None, :]
    positions = jnp.arange(width_rows)
    earlier = positions[:, None] > positions[None, :]
    order_within = jnp.sum((shared & earlier).astype(jnp.int32), axis=1)
    return (partner * capacity + order_within, target_row)


def move_any(rows_next, migration_plan):
    width_rows = rows_next.shape[0]
    devices_along = lax.axis_size("rve")
    peers_used = min(devices_along // 2, width_rows // 2)
    capacity = width_rows // peers_used
    total = devices_along * capacity
    slot_index, target_row = route_slots(migration_plan, width_rows, capacity)
    matches = slot_index[None, :] == jnp.arange(total)[:, None]
    source = jnp.sum(jnp.where(matches, jnp.arange(width_rows)[None, :], 0), axis=1)
    labels = jnp.sum(jnp.where(matches, target_row[None, :] + 1, 0), axis=1)
    outgoing = jnp.take(rows_next, source, axis=0)
    arrived = lax.all_to_all(outgoing, "rve", split_axis=0, concat_axis=0, tiled=True)
    tags = lax.all_to_all(labels, "rve", split_axis=0, concat_axis=0, tiled=True)
    wanted = tags[None, :] == jnp.arange(1, width_rows + 1)[:, None]
    place = jnp.sum(jnp.where(wanted, jnp.arange(total)[None, :], 0), axis=1)
    return jnp.take(arrived, place, axis=0)


def in_hbm(value):
    return pltpu.with_memory_space_constraint(value, pltpu.HBM)


def in_vmem(value):
    return pltpu.with_memory_space_constraint(value, pltpu.VMEM)


def on_device(displacement, plastic, bulk, shear, radius, counts, migration_plan):
    layers = lax.axis_size("rve")
    columns = lax.axis_size("mic") * lax.axis_size("mac")
    lay = Layout(plastic.shape, displacement.shape[3], layers, columns)
    fast = layers <= 2 + len(lay.near)
    if not fast:
        lay.near = []
    rows, extent, wide, n = lay.rows, lay.extent, lay.wide, len(lay.near)
    f32 = jnp.float32
    tiles = wide // 128
    fixed = [bulk, shear, radius, jnp.asarray(symbol_table(extent)), jnp.asarray(plane_tables(extent))]
    vmem = pl.BlockSpec(memory_space=pltpu.VMEM)
    anywhere = pl.BlockSpec(memory_space=pl.ANY)
    sem = pltpu.SemaphoreType.DMA
    params = pltpu.CompilerParams(vmem_limit_bytes=VMEM_BYTES)
    staging = pltpu.VMEM((tiles, rows * lay.step, 128), f32)
    small = pltpu.SMEM((rows,), jnp.int32)
    plan = in_hbm(migration_plan)
    nodes, state, *rest = pl.pallas_call(
        lambda *refs: pack_kernel(lay, *refs),
        out_shape=[pltpu.VMEM((8, 128), f32), staging]
        + [pltpu.VMEM(v.shape, v.dtype) for v in fixed]
        + [pltpu.VMEM((lay.early, lay.step, wide), f32)] * n,
        in_specs=[anywhere] * 8,
        out_specs=[vmem] * (7 + n),
        scratch_shapes=[
            small,
            pltpu.VMEM(displacement.shape, f32),
            sem((2,)),
            sem((max(n, 1), max(lay.early, 1))),
            sem((5,)),
            sem((rows, tiles)),
        ],
        name="pack",
    )(in_hbm(displacement), plan, in_hbm(plastic.reshape(rows, lay.step, wide)), *[in_hbm(v) for v in fixed])
    fixed = [in_vmem(v) for v in rest[:5]]
    raw = rest[5:]
    upper = ring(nodes, -1)
    for i, offset in enumerate(lay.near):
        raw[i] = ring(raw[i], offset)
    both = jnp.concatenate([nodes, upper], axis=0)
    side = sideways(both, -1)
    nodes, upper = in_vmem(nodes), in_vmem(upper)
    outs = [staging, pltpu.VMEM((8 + lay.meta, 128), f32)]
    outs += [pltpu.VMEM((lay.meta, 128), f32)] * (n - 1)
    outs += [pltpu.VMEM((lay.late, lay.step, wide), f32)] * n
    finished, *rest = pl.pallas_call(
        lambda *refs: source_kernel(lay, *refs),
        out_shape=outs,
        in_specs=[vmem] * 3 + [anywhere] * 2 + [vmem] * 6,
        out_specs=[vmem] * len(outs),
        scratch_shapes=[small, small, sem((2,)), sem((max(n, 1), max(lay.late, 1), tiles))]
        + solve_scratch(extent, rows),
        compiler_params=params,
        name="solve_source",
    )(nodes, upper, in_vmem(side), in_hbm(counts), plan, in_vmem(state), *fixed)
    first, others, done = rest[0], rest[1:n], rest[max(n, 1) :]
    below = ring(first, 1)
    notes = [below]
    for i, offset in enumerate(lay.near[1:]):
        notes.append(ring(others[i], offset))
    for i, offset in enumerate(lay.near):
        done[i] = ring(done[i], offset)
    pair = jnp.concatenate([first[:8], below[:8]], axis=0)
    beside = sideways(pair, 1)
    force = pl.pallas_call(
        lambda *refs: force_kernel(lay, *refs),
        out_shape=jax.ShapeDtypeStruct(displacement.shape, f32),
        in_specs=[vmem] * 3,
        out_specs=vmem,
        name="force",
    )(in_vmem(first), in_vmem(below), in_vmem(beside))

    def unusual(_):
        rows_first = finished.reshape(tiles, rows, lay.step, 128).transpose(1, 2, 0, 3)
        return move_any(rows_first.reshape(rows, lay.step, wide), migration_plan)

    if not fast:
        return force, unusual(None).reshape(plastic.shape)
    notes = [in_vmem(v) for v in notes]
    marks = [pltpu.SMEM(v.shape, f32) for v in notes]
    arrived, rare = pl.pallas_call(
        lambda *refs: target_kernel(lay, *refs),
        out_shape=[pltpu.HBM((rows, lay.step, wide), f32), jax.ShapeDtypeStruct((8, 128), f32)],
        in_specs=[vmem] * n + [vmem] * n + [vmem] * 7,
        out_specs=[anywhere, vmem],
        scratch_shapes=marks
        + [staging, staging, sem((rows, tiles)), sem((rows, tiles)), sem((n,))]
        + [pltpu.VMEM((rows, 128), f32)]
        + solve_scratch(extent, rows),
        compiler_params=params,
        name="solve_target",
    )(*notes, *[in_vmem(v) for v in raw], nodes, upper, *fixed)
    moved = pl.pallas_call(
        lambda *refs: place_kernel(lay, *refs),
        out_shape=pltpu.HBM((rows, lay.step, wide), f32),
        in_specs=[vmem] * (2 * n) + [anywhere, vmem, anywhere],
        out_specs=anywhere,
        scratch_shapes=marks
        + [small, sem((n + 1,)), sem((n, lay.late)), sem((rows, tiles))],
        input_output_aliases={2 * n + 2: 0},
        compiler_params=params,
        name="place",
    )(*notes, *[in_vmem(v) for v in done], plan, in_vmem(finished), in_hbm(arrived))
    moved = lax.cond(rare[0, 0] > 0.0, unusual, lambda v: v, moved)
    return force, moved.reshape(plastic.shape)


def solution(mesh):
    everyone = ("rve", "mic", "mac")

    return jax.shard_map(
        on_device,
        mesh=mesh,
        in_specs=(
            P(None, "rve", ("mic", "mac"), None),
            P(everyone, None, None, None),
            P(), P(), P(),
            P(everyone),
            P(everyone),
        ),
        out_specs=(P(None, "rve", ("mic", "mac"), None), P(everyone, None, None, None)),
        check_vma=False,
    )
```

```python
import math

import jax
import jax.numpy as jnp
import numpy as np
from jax import lax
from jax.experimental import pallas as pl
from jax.experimental.pallas import tpu as pltpu
from jax.sharding import PartitionSpec as P


COUPLING = 0.7
EARLY = 2
VMEM_BYTES = 20 * 2**20
PAIRS = [(0, 0), (1, 1), (2, 2), (1, 2), (0, 2), (0, 1)]
SYM = [(m, n) for m in range(6) for n in range(m, 6)]


def symbol_table(extent):
    wave = ((np.arange(extent) + extent // 2) % extent - extent // 2).astype(np.float64)
    grid = np.meshgrid(wave, wave, wave, indexing="ij")
    square = grid[0] ** 2 + grid[1] ** 2 + grid[2] ** 2
    live = square > 0
    safe = np.where(live, square, 1.0)
    full = np.zeros((6, 6) + square.shape)
    for n, (p, q) in enumerate(PAIRS):
        traction = [np.zeros_like(square) for _ in range(3)]
        traction[p] = traction[p] + grid[q]
        if p != q:
            traction[q] = traction[q] + grid[p]
        normal = sum(grid[i] * traction[i] for i in range(3))
        weight = 1.0 if p == q else 2.0
        for m, (i, j) in enumerate(PAIRS):
            value = (grid[j] * traction[i] + grid[i] * traction[j]) / (2.0 * safe)
            value = value - COUPLING * grid[i] * grid[j] * normal / safe**2
            full[m, n] = np.where(live, value, 0.0) / weight
    flip = (-np.arange(extent)) % extent
    mirrored = full[:, :, flip][:, :, :, flip][:, :, :, :, flip]
    real = 0.5 * (full + mirrored) / extent**3
    half = extent // 2
    scale = np.where((np.arange(half + 1) % half) == 0, 1.0, 2.0).reshape(-1, 1)
    table = np.zeros((len(SYM), extent, extent * extent))
    for index, (m, n) in enumerate(SYM):
        table[index, : half + 1] = real[m, n, : half + 1].reshape(half + 1, -1) * scale
    return table.astype(np.float32)


def plane_tables(extent):
    plane = np.arange(extent * extent)
    row, col = plane // extent, plane % extent
    phase = (row[:, None] * row[None, :] + col[:, None] * col[None, :]) % extent
    angle = 2.0 * np.pi * phase / extent
    out = []
    for value in (np.cos(angle) + np.sin(angle), np.cos(angle) - np.sin(angle)):
        value = value.astype(np.float32)
        high = value.astype(jnp.bfloat16)
        low = (value - high.astype(np.float32)).astype(jnp.bfloat16)
        out.append(np.concatenate([high, high, low], axis=0))
    return np.stack(out)


C1, C2, C3 = math.cos(math.pi / 8), math.cos(math.pi / 4), math.cos(3 * math.pi / 8)


def cosine_sums(first, s, last):
    p = [s[j - 1] + s[7 - j] for j in (1, 2, 3)]
    m = [s[j - 1] - s[7 - j] for j in (1, 2, 3)]
    mid = s[3]
    total, diff = first + last, first - last
    t = m[1] * C2
    u, v = diff + t, diff - t
    w1 = m[0] * C1 + m[2] * C3
    w3 = m[0] * C3 - m[2] * C1
    plus, minus = total + mid, total - mid
    outer, inner = p[0] + p[2], (p[0] - p[2]) * C2
    even = plus + p[1]
    return [
        even + outer, u + w1, minus + inner, v + w3, plus - p[1],
        v - w3, minus - inner, u - w1, even - outer,
    ]


def sine_sums(d):
    n = [d[j - 1] + d[7 - j] for j in (1, 2, 3)]
    r = [d[j - 1] - d[7 - j] for j in (1, 2, 3)]
    mid = d[3]
    y1 = n[0] * C3 + n[2] * C1
    y3 = n[0] * C1 - n[2] * C3
    g = n[1] * C2
    gp, gm = g + mid, g - mid
    e = (r[0] + r[2]) * C2
    return [y1 + gp, e + r[1], y3 + gm, r[0] - r[2], y3 - gm, e - r[1], y1 - gp]


def split_dot(x, weights):
    high = x.astype(jnp.bfloat16)
    low = (x - high.astype(jnp.float32)).astype(jnp.bfloat16)
    stacked = jnp.concatenate([high, low, high], axis=1)
    return jnp.dot(stacked, weights, preferred_element_type=jnp.float32)


def elastic_parts(strain, plastic, shear2):
    elastic = [strain[c] - plastic[c] for c in range(6)]
    volume = elastic[0] + elastic[1] + elastic[2]
    mean = volume * (1.0 / 3.0)
    dev = [elastic[c] - mean for c in range(3)] + elastic[3:]
    normal = dev[0] * dev[0] + dev[1] * dev[1] + dev[2] * dev[2]
    shear = dev[3] * dev[3] + dev[4] * dev[4] + dev[5] * dev[5]
    size = (normal + (shear + shear)) * (shear2 * shear2)
    return volume, dev, size


def solve(extent, rows, state, out, strain_cols, late_counts, consts, scratch, ship=None):
    table_ref, plane_ref = consts
    bulk_ref, shear_ref, radius_ref = [table_ref.at[len(SYM) + i] for i in range(3)]
    e_ref, u_ref, a_ref, b_ref, a2_ref, b2_ref, t_ref = scratch
    half = extent // 2
    wide = extent * extent
    lanes = 128
    group = 6 * rows

    for c in range(6):
        column = jnp.broadcast_to(strain_cols[c], (rows, wide))
        for a in range(extent):
            e_ref[c, a] = column
            u_ref[0, c, a] = jnp.zeros((rows, wide), jnp.float32)
            u_ref[1, c, a] = jnp.zeros((rows, wide), jnp.float32)
    count_col, top_count = late_counts()

    def current(a, tile, k, alpha, beta):
        lane = pl.ds(tile * lanes, lanes)
        newer, older = (k + 1) & 1, k & 1
        values = []
        for c in range(6):
            v = e_ref[c, a, :, lane] - alpha * u_ref[newer, c, a, :, lane]
            values.append(v - beta * u_ref[older, c, a, :, lane])
        plastic = [state[c, a, :, lane] for c in range(6)]
        shear2 = 2.0 * shear_ref[pl.ds(a, 1), lane]
        radius = radius_ref[pl.ds(a, 1), lane]
        bulk = bulk_ref[pl.ds(a, 1), lane]
        volume, dev, size = elastic_parts(values, plastic, shear2)
        factor = radius * lax.rsqrt(jnp.maximum(size, radius * radius))
        gain = factor * shear2
        pressure = bulk * volume
        stress = [gain * dev[c] + pressure for c in range(3)]
        stress += [gain * dev[c] for c in range(3, 6)]
        return values, plastic, dev, factor, stress

    def sweep(k, carry):
        alpha, beta, before = carry
        for a in range(extent):
            for tile in range(wide // lanes):
                lane = pl.ds(tile * lanes, lanes)
                values, _, _, _, stress = current(a, tile, k, alpha, beta)
                for c in range(6):
                    e_ref[c, a, :, lane] = values[c]
                    t_ref[c, a, :, lane] = stress[c]
        for c in range(6):
            for tile in range(wide // lanes):
                lane = pl.ds(tile * lanes, lanes)
                x = [t_ref[c, a, :, lane] for a in range(extent)]
                s = [x[j] + x[extent - j] for j in range(1, half)]
                d = [x[j] - x[extent - j] for j in range(1, half)]
                for kk, value in enumerate(cosine_sums(x[0], s, x[half])):
                    a_ref[pl.ds(kk * group + c * rows, rows), lane] = value
                for kk, value in enumerate(sine_sums(d)):
                    b_ref[pl.ds(kk * group + c * rows, rows), lane] = value
        a2_ref[...] = split_dot(a_ref[...], plane_ref[0])
        b2_ref[...] = split_dot(b_ref[...], plane_ref[1])
        for kk in range(half + 1):
            ends = kk == 0 or kk == half
            for tile in range(wide // lanes):
                lane = pl.ds(tile * lanes, lanes)
                coef = {}
                for index, pair in enumerate(SYM):
                    coef[pair] = table_ref[index, pl.ds(kk, 1), lane]
                    coef[pair[::-1]] = coef[pair]

                def place(c, odd):
                    if ends:
                        return a2_ref, a_ref, pl.ds(kk * group + c * rows, rows)
                    if (c >= 4) != odd:
                        return b2_ref, b_ref, pl.ds((kk - 1) * group + c * rows, rows)
                    return a2_ref, a_ref, pl.ds(kk * group + c * rows, rows)

                for odd in (False,) if ends else (False, True):
                    tau = []
                    for c in range(6):
                        src, _, where = place(c, odd)
                        value = src[where, lane]
                        tau.append(value if c < 3 else value + value)
                    for m in range(6):
                        acc = coef[m, 0] * tau[0]
                        for n in range(1, 6):
                            acc = acc + coef[m, n] * tau[n]
                        _, dst, where = place(m, odd)
                        dst[where, lane] = acc
        a2_ref[...] = split_dot(a_ref[...], plane_ref[0])
        b2_ref[...] = split_dot(b_ref[...], plane_ref[1])
        num = jnp.zeros((rows, lanes), jnp.float32)
        den = jnp.zeros((rows, lanes), jnp.float32)
        newest, last = k & 1, (k + 1) & 1
        for c in range(6):
            for tile in range(wide // lanes):
                lane = pl.ds(tile * lanes, lanes)
                ca = [a2_ref[pl.ds(kk * group + c * rows, rows), lane] for kk in range(half + 1)]
                sb = [b2_ref[pl.ds(kk * group + c * rows, rows), lane] for kk in range(half - 1)]
                even = cosine_sums(ca[0], ca[1:half], ca[half])
                odd = [None] + sine_sums(sb)
                for a in range(extent):
                    j = min(a, extent - a)
                    if a == 0 or a == half:
                        value = even[j]
                    elif a < half:
                        value = even[j] + odd[j]
                    else:
                        value = even[j] - odd[j]
                    change = value - u_ref[last, c, a, :, lane]
                    num = num + change * value
                    den = den + change * change
                    u_ref[newest, c, a, :, lane] = value
        scale = 1.0 / (6 * extent**3)
        top = jnp.sum(num, axis=1, keepdims=True) * scale
        bottom = jnp.sum(den, axis=1, keepdims=True) * scale + 1e-06
        weight = jnp.where(k > 0, top / bottom, 0.0)
        active = jnp.where(count_col > k.astype(jnp.float32), 1.0, 0.0)
        alpha = active * (1.0 - weight)
        beta = active * weight * before
        spread = lambda v: jnp.broadcast_to(v, (rows, lanes))
        return spread(alpha), spread(beta), weight

    zero = jnp.zeros((rows, lanes), jnp.float32)
    alpha, beta, _ = lax.fori_loop(
        0, top_count, sweep, (zero, zero, jnp.zeros((rows, 1), jnp.float32))
    )
    sums = [jnp.zeros((rows, lanes), jnp.float32) for _ in range(6)]
    for a in range(extent):
        for tile in range(wide // lanes):
            lane = pl.ds(tile * lanes, lanes)
            _, plastic, dev, factor, stress = current(a, tile, top_count, alpha, beta)
            rest = 1.0 - factor
            for c in range(6):
                sums[c] = sums[c] + stress[c]
                out[c, a, :, lane] = plastic[c] + rest * dev[c]
        if ship and a % half == half - 1:
            ship(a // half)
    return sums


def solve_scratch(extent, rows):
    half, wide = extent // 2, extent * extent
    field = (6, extent, rows, wide)
    f32 = jnp.float32
    return [
        pltpu.VMEM(field, f32),
        pltpu.VMEM((2,) + field, f32),
        pltpu.VMEM(((half + 1) * 6 * rows, wide), f32),
        pltpu.VMEM(((half - 1) * 6 * rows, wide), f32),
        pltpu.VMEM(((half + 1) * 6 * rows, wide), f32),
        pltpu.VMEM(((half - 1) * 6 * rows, wide), f32),
        pltpu.VMEM(field, f32),
    ]


def to_column(row, mask):
    return jnp.sum(jnp.where(mask, jnp.broadcast_to(row, mask.shape), 0.0), axis=1, keepdims=True)


def to_row(column, mask):
    return jnp.sum(jnp.where(mask, jnp.broadcast_to(column, mask.shape), 0.0), axis=0, keepdims=True)


def counts_column(counts, rows):
    where = lax.broadcasted_iota(jnp.int32, (rows, 1), 0)
    column = jnp.zeros((rows, 1), jnp.float32)
    top = counts[0]
    for r in range(rows):
        column = jnp.where(where == r, counts[r].astype(jnp.float32), column)
        top = jnp.maximum(top, counts[r])
    return column, top


def lane_mask(rows):
    shape = (rows, 128)
    return lax.broadcasted_iota(jnp.int32, shape, 0) == lax.broadcasted_iota(jnp.int32, shape, 1)


def spread_nodes(value):
    return value, pltpu.roll(value, 127, 1)


def strain_rows(corners):
    pairs = [spread_nodes(v) for v in corners]
    total = [lo + hi for lo, hi in pairs]
    rise = [hi - lo for lo, hi in pairs]
    h = [
        0.25 * ((total[1] + total[3]) - (total[0] + total[2])),
        0.25 * ((total[2] + total[3]) - (total[0] + total[1])),
        0.25 * ((rise[0] + rise[1]) + (rise[2] + rise[3])),
    ]
    pick = lambda i, j: h[j][i : i + 1]
    return [
        pick(0, 0), pick(1, 1), pick(2, 2),
        0.5 * (pick(1, 2) + pick(2, 1)),
        0.5 * (pick(0, 2) + pick(2, 0)),
        0.5 * (pick(0, 1) + pick(1, 0)),
    ]


def zero_below(value):
    return value, pltpu.roll(value, 1, 1)


def node_force(own, low_a, low_b, low_ab):
    total, rise = [], []
    for value in (own, low_a, low_b, low_ab):
        value, below = zero_below(value)
        total.append(value + below)
        rise.append(below - value)
    along = [
        (total[1] + total[3]) - (total[0] + total[2]),
        (total[2] + total[3]) - (total[0] + total[1]),
        (rise[0] + rise[1]) + (rise[2] + rise[3]),
    ]
    index = [[0, 5, 4], [5, 1, 3], [4, 3, 2]]
    rows = []
    for i in range(3):
        parts = [along[j][index[i][j] : index[i][j] + 1] for j in range(3)]
        rows.append(0.25 * (parts[0] + parts[1] + parts[2]))
    return rows


class Layout:
    def __init__(self, plastic_shape, depth, layers, columns):
        self.rows, _, self.extent, self.wide = plastic_shape
        self.depth, self.layers, self.columns = depth, layers, columns
        self.peers = min(layers // 2, self.rows // 2)
        self.capacity = self.rows // self.peers
        self.near = [k for k in (1, 2) if k < layers]
        self.early = (self.capacity * EARLY) // 4
        self.late = self.capacity - self.early
        self.row = (6, self.extent, self.wide)
        self.field = (6, self.extent, self.rows, self.wide)
        self.meta = -(-self.capacity // 8) * 8

    def route(self, plan):
        here = lax.axis_index("rve")
        block = self.rows * self.columns
        partner = [lax.div(plan[e], block) for e in range(self.rows)]
        away = []
        for p in partner:
            d = p - here
            away.append(jnp.where(d < 0, d + self.layers, d))
        order = []
        for e in range(self.rows):
            before = jnp.int32(0)
            for f in range(e):
                before = before + (away[f] == away[e]).astype(jnp.int32)
            order.append(before)
        target = [lax.rem(plan[e], self.rows) for e in range(self.rows)]
        return away, order, target

    def late_slots(self):
        places = range(self.early, self.capacity)
        return [(i, s) for i in range(len(self.near)) for s in places]

    def pick(self, away, order, offset, place):
        row, found = jnp.int32(0), jnp.int32(0)
        for e in range(self.rows):
            hit = jnp.logical_and(away[e] == offset, order[e] == place)
            row = jnp.where(hit, e, row)
            found = jnp.where(hit, 1, found)
        return row, found


def pack_kernel(lay, *refs):
    displacement, plan, counts, plastic = refs[:4]
    plane, table, *fields = refs[4:9]
    nodes, state, plane_copy, board, plan_s, counts_s = refs[9:15]
    boxes = refs[15 : 15 + len(lay.near)]
    corner, small_sems, box_sems, fix_sems, row_sems = refs[15 + len(lay.near) :]
    load_plan = pltpu.make_async_copy(plan, plan_s, small_sems.at[0])
    load_plan.start()
    load_corner = pltpu.make_async_copy(displacement, corner, small_sems.at[1])
    load_corner.start()
    copies = [pltpu.make_async_copy(counts, counts_s, small_sems.at[2])]
    copies[0].start()
    for r in range(lay.rows):
        copies.append(pltpu.make_async_copy(plastic.at[r], state.at[:, :, r, :], row_sems.at[r]))
        copies[-1].start()
    nodes[...] = jnp.zeros(nodes.shape, jnp.float32)
    load_plan.wait()
    away, order, _ = lay.route(plan_s)
    packed = []
    for i, offset in enumerate(lay.near):
        for s in range(lay.early):
            row, _ = lay.pick(away, order, offset, s)
            packed.append(pltpu.make_async_copy(plastic.at[row], boxes[i].at[s], box_sems.at[i, s]))
            packed[-1].start()
    fixed = [(plane, plane_copy), (table, board.at[pl.ds(0, len(SYM))])]
    fixed += [(field, board.at[len(SYM) + i]) for i, field in enumerate(fields)]
    for i, (src, dst) in enumerate(fixed):
        copies.append(pltpu.make_async_copy(src, dst, fix_sems.at[i]))
        copies[-1].start()
    load_corner.wait()
    for i in range(3):
        nodes[i : i + 1, : lay.depth] = corner[i, 0]
    rare = jnp.int32(0)
    for e in range(lay.rows):
        usual = away[e] == 0
        for offset in lay.near:
            usual = jnp.logical_or(usual, away[e] == offset)
        rare = jnp.where(usual, rare, 1)
    nodes[3:4] = jnp.full((1, 128), rare.astype(jnp.float32))
    for copy in copies + packed:
        copy.wait()


def source_kernel(lay, *refs):
    extent, rows = lay.extent, lay.rows
    own, upper, side, counts_s, plan_s, state, plane, board = refs[:8]
    n = len(lay.near)
    finished, first = refs[8:10]
    others = refs[10 : 9 + n]
    at = 9 + max(n, 1)
    boxes = refs[at : at + n]
    box_sems = refs[at + n]
    scratch = refs[at + n + 1 :]
    mask = lane_mask(rows)
    inside = jnp.where(lax.axis_index("rve") < lay.layers - 1, 1.0, 0.0)
    corners = [own[0:3], upper[0:3] * inside, side[0:3], side[8:11] * inside]
    strain = [to_column(v, mask) for v in strain_rows(corners)]
    column, top = counts_column(counts_s, rows)
    away, order, target = lay.route(plan_s)
    stores = []

    def ship(part):
        span = pl.ds(part * (extent // 2), extent // 2)
        for i, offset in enumerate(lay.near):
            for s in range(lay.late):
                row, _ = lay.pick(away, order, offset, lay.early + s)
                src = finished.at[:, span, row, :]
                dst = boxes[i].at[s, :, span, :]
                stores.append(pltpu.make_async_copy(src, dst, box_sems.at[i, s, part]))
                stores[-1].start()

    sums = solve(
        extent, rows, state, finished, strain, lambda: (column, top),
        (board, plane), scratch, ship,
    )
    lane = lax.broadcasted_iota(jnp.int32, (rows, 128), 1)
    sub = lax.broadcasted_iota(jnp.int32, (rows, 128), 0)
    card = jnp.zeros((rows, 128), jnp.float32)
    for c in range(6):
        card = jnp.where(lane == c, strain[c], card)
    card = jnp.where(lane == 6, column, card)
    for r in range(rows):
        label = (target[r] + 1).astype(jnp.float32)
        card = jnp.where(jnp.logical_and(lane == 7, sub == r), label, card)
    notes = (first,) + tuple(others)
    first[...] = jnp.zeros(first.shape, jnp.float32)
    for i, offset in enumerate(lay.near):
        base = 8 if i == 0 else 0
        if i:
            notes[i][...] = jnp.zeros(notes[i].shape, jnp.float32)
        for s in range(lay.capacity):
            row, found = lay.pick(away, order, offset, s)
            chosen = jnp.logical_and(sub == row, found > 0)
            line = jnp.sum(jnp.where(chosen, card, 0.0), axis=0, keepdims=True)
            line = jnp.where(lane[0:1] == 8, jnp.maximum(own[3:4], upper[3:4]), line)
            notes[i][base + s : base + s + 1] = line
    for c in range(6):
        mean = jnp.sum(sums[c], axis=1, keepdims=True) * (1.0 / extent**3)
        first[c : c + 1] = to_row(mean, mask)
    for copy in stores:
        copy.wait()


def note_row(i, s):
    return (8 if i == 0 else 0) + s


def target_kernel(lay, *refs):
    extent, rows, n = lay.extent, lay.rows, len(lay.near)
    notes, boxes = refs[:n], refs[n : 2 * n]
    upper, plan_s, plane, board = refs[2 * n : 2 * n + 4]
    arrived, rare_out, goals = refs[2 * n + 4 : 2 * n + 7]
    rest = refs[2 * n + 7 :]
    marks, rest = rest[:n], rest[n:]
    stage, result, load_sems, store_sems, mark_sems, cards, upper_s = rest[:7]
    scratch = rest[7:]
    slots = [(i, s) for i in range(n) for s in range(lay.early)]
    reads = [pltpu.make_async_copy(notes[i], marks[i], mark_sems.at[i]) for i in range(n)]
    reads.append(pltpu.make_async_copy(upper, upper_s, mark_sems.at[n]))
    loads = []
    for r, (i, s) in enumerate(slots):
        dst = stage.at[:, :, r, :]
        loads.append(pltpu.make_async_copy(boxes[i].at[s], dst, load_sems.at[r]))
    for copy in reads + loads:
        copy.start()
    cards[...] = jnp.zeros(cards.shape, jnp.float32)
    for r, (i, s) in enumerate(slots):
        cards[r : r + 1] = notes[i][note_row(i, s) : note_row(i, s) + 1]
    card = cards[...]
    strain = [card[:, c : c + 1] for c in range(6)]

    def late_counts():
        for copy in reads:
            copy.wait()
        most = jnp.float32(0.0)
        for i, s in slots:
            most = jnp.maximum(most, marks[i][note_row(i, s), 6])
        away, _, target = lay.route(plan_s)
        for index, (i, s) in enumerate(lay.late_slots()):
            goals[index] = marks[i][note_row(i, s), 7].astype(jnp.int32) - 1
        for e in range(rows):
            goals[n * lay.late + e] = jnp.where(away[e] == 0, target[e], -1)
        rare = jnp.maximum(marks[0][note_row(0, 0), 8], marks[n - 1][note_row(n - 1, 0), 8])
        rare_out[0] = jnp.where(jnp.maximum(rare, upper_s[3, 0]) > 0.0, 1, 0)
        return card[:, 6:7], most.astype(jnp.int32)

    for copy in loads:
        copy.wait()
    solve(
        extent, rows, stage, result, strain, late_counts,
        (board, plane), scratch,
    )
    moves = []
    for r, (i, s) in enumerate(slots):
        label = marks[i][note_row(i, s), 7].astype(jnp.int32)
        moves.append((r, label > 0, jnp.maximum(label - 1, 0)))
    for phase in ("start", "wait"):
        for r, valid, where in moves:

            @pl.when(valid)
            def _(r=r, where=where, phase=phase):
                src = result.at[:, :, r, :]
                copy = pltpu.make_async_copy(src, arrived.at[where], store_sems.at[r])
                getattr(copy, phase)()


def place_kernel(lay, *refs):
    n = len(lay.near)
    goals, boxes = refs[0], refs[1 : n + 1]
    finished, _, out, sems = refs[n + 1 :]
    sources = [boxes[i].at[s - lay.early] for i, s in lay.late_slots()]
    sources += [finished.at[:, :, e, :] for e in range(lay.rows)]
    for phase in ("start", "wait"):
        for index, src in enumerate(sources):

            @pl.when(goals[index] >= 0)
            def _(index=index, src=src, phase=phase):
                where = jnp.maximum(goals[index], 0)
                getattr(pltpu.make_async_copy(src, out.at[where], sems.at[index]), phase)()


def force_kernel(lay, own, below, side, out):
    inside = jnp.where(lax.axis_index("rve") > 0, 1.0, 0.0)
    rows = node_force(own[0:6], below[0:6] * inside, side[0:6], side[8:14] * inside)
    for i in range(3):
        out[i, 0] = rows[i][:, : lay.depth]


def shift_pairs(counts, steps):
    pairs = []
    for flat in range(math.prod(counts)):
        at, rest = [], flat
        for size in reversed(counts):
            at.insert(0, rest % size)
            rest //= size
        to = [p + s for p, s in zip(at, steps)]
        if all(0 <= t < size for t, size in zip(to, counts)):
            target = 0
            for t, size in zip(to, counts):
                target = target * size + t
            pairs.append((flat, target))
    return pairs


def ring(value, step):
    layers = lax.axis_size("rve")
    return lax.ppermute(value, "rve", [(i, (i + step) % layers) for i in range(layers)])


def sideways(value, step):
    columns = lax.axis_size("mic") * lax.axis_size("mac")
    return lax.ppermute(value, ("mic", "mac"), shift_pairs([columns], [step]))


def route_slots(migration_plan, width_rows, capacity):
    columns = lax.axis_size("mic") * lax.axis_size("mac")
    partner = migration_plan // width_rows // columns
    target_row = migration_plan % width_rows
    shared = partner[:, None] == partner[None, :]
    positions = jnp.arange(width_rows)
    earlier = positions[:, None] > positions[None, :]
    order_within = jnp.sum((shared & earlier).astype(jnp.int32), axis=1)
    return (partner * capacity + order_within, target_row)


def move_any(rows_next, migration_plan):
    width_rows = rows_next.shape[0]
    devices_along = lax.axis_size("rve")
    peers_used = min(devices_along // 2, width_rows // 2)
    capacity = width_rows // peers_used
    total = devices_along * capacity
    slot_index, target_row = route_slots(migration_plan, width_rows, capacity)
    matches = slot_index[None, :] == jnp.arange(total)[:, None]
    source = jnp.sum(jnp.where(matches, jnp.arange(width_rows)[None, :], 0), axis=1)
    labels = jnp.sum(jnp.where(matches, target_row[None, :] + 1, 0), axis=1)
    outgoing = jnp.take(rows_next, source, axis=0)
    arrived = lax.all_to_all(outgoing, "rve", split_axis=0, concat_axis=0, tiled=True)
    tags = lax.all_to_all(labels, "rve", split_axis=0, concat_axis=0, tiled=True)
    wanted = tags[None, :] == jnp.arange(1, width_rows + 1)[:, None]
    place = jnp.sum(jnp.where(wanted, jnp.arange(total)[None, :], 0), axis=1)
    return jnp.take(arrived, place, axis=0)


def in_hbm(value):
    return pltpu.with_memory_space_constraint(value, pltpu.HBM)


def in_vmem(value):
    return pltpu.with_memory_space_constraint(value, pltpu.VMEM)


def on_device(displacement, plastic, bulk, shear, radius, counts, migration_plan):
    layers = lax.axis_size("rve")
    columns = lax.axis_size("mic") * lax.axis_size("mac")
    lay = Layout(plastic.shape, displacement.shape[3], layers, columns)
    fast = layers <= 2 + len(lay.near)
    if not fast:
        lay.near = []
    rows, extent, wide, n = lay.rows, lay.extent, lay.wide, len(lay.near)
    f32 = jnp.float32
    plane = jnp.asarray(plane_tables(extent))
    fixed = [plane, jnp.asarray(symbol_table(extent)), bulk, shear, radius]
    vmem = pl.BlockSpec(memory_space=pltpu.VMEM)
    anywhere = pl.BlockSpec(memory_space=pl.ANY)
    smem = pl.BlockSpec(memory_space=pltpu.SMEM)
    sem = pltpu.SemaphoreType.DMA
    params = pltpu.CompilerParams(vmem_limit_bytes=VMEM_BYTES)
    staging = pltpu.VMEM(lay.field, f32)
    small = pltpu.SMEM((rows,), jnp.int32)
    plan = in_hbm(migration_plan)
    nodes, state, *rest = pl.pallas_call(
        lambda *refs: pack_kernel(lay, *refs),
        out_shape=[pltpu.VMEM((8, 128), f32), staging]
        + [pltpu.VMEM(plane.shape, plane.dtype), pltpu.VMEM((len(SYM) + 3, extent, wide), f32)]
        + [small, small]
        + [pltpu.VMEM((lay.early,) + lay.row, f32)] * n,
        in_specs=[anywhere] * 9,
        out_specs=[vmem] * 4 + [smem] * 2 + [vmem] * n,
        scratch_shapes=[
            pltpu.VMEM(displacement.shape, f32),
            sem((3,)),
            sem((max(n, 1), max(lay.early, 1))),
            sem((5,)),
            sem((rows,)),
        ],
        name="pack",
    )(in_hbm(displacement), plan, in_hbm(counts), in_hbm(plastic), *[in_hbm(v) for v in fixed])
    fixed = [in_vmem(v) for v in rest[:2]]
    plan, counts = [pltpu.with_memory_space_constraint(v, pltpu.SMEM) for v in rest[2:4]]
    raw = rest[4:]
    upper = ring(nodes, -1)
    for i, offset in enumerate(lay.near):
        raw[i] = ring(raw[i], offset)
    both = jnp.concatenate([nodes, upper], axis=0)
    side = sideways(both, -1)
    nodes, upper = in_vmem(nodes), in_vmem(upper)
    outs = [staging, pltpu.VMEM((8 + lay.meta, 128), f32)]
    outs += [pltpu.VMEM((lay.meta, 128), f32)] * (n - 1)
    outs += [pltpu.HBM((lay.late,) + lay.row, f32)] * n
    finished, *rest = pl.pallas_call(
        lambda *refs: source_kernel(lay, *refs),
        out_shape=outs,
        in_specs=[vmem] * 3 + [smem] * 2 + [vmem] * 3,
        out_specs=[vmem] * (1 + max(n, 1)) + [anywhere] * n,
        scratch_shapes=[sem((max(n, 1), max(lay.late, 1), 2))]
        + solve_scratch(extent, rows),
        compiler_params=params,
        name="solve_source",
    )(nodes, upper, in_vmem(side), counts, plan, in_vmem(state), *fixed)
    first, others, done = rest[0], rest[1:n], rest[max(n, 1) :]
    below = ring(first, 1)
    notes = [below]
    for i, offset in enumerate(lay.near[1:]):
        notes.append(ring(others[i], offset))
    for i, offset in enumerate(lay.near):
        done[i] = ring(done[i], offset)
    pair = jnp.concatenate([first[:8], below[:8]], axis=0)
    beside = sideways(pair, 1)
    force = pl.pallas_call(
        lambda *refs: force_kernel(lay, *refs),
        out_shape=jax.ShapeDtypeStruct(displacement.shape, f32),
        in_specs=[vmem] * 3,
        out_specs=vmem,
        name="force",
    )(in_vmem(first), in_vmem(below), in_vmem(beside))

    def unusual(_):
        return move_any(finished.transpose(2, 0, 1, 3), migration_plan)

    if not fast:
        return force, unusual(None)
    notes = [in_vmem(v) for v in notes]
    total = n * lay.late + rows
    arrived, rare, goals = pl.pallas_call(
        lambda *refs: target_kernel(lay, *refs),
        out_shape=[
            pltpu.HBM(plastic.shape, f32),
            pltpu.SMEM((1,), jnp.int32),
            pltpu.SMEM((total,), jnp.int32),
        ],
        in_specs=[vmem] * (2 * n + 1) + [smem] + [vmem] * 2,
        out_specs=[anywhere, smem, smem],
        scratch_shapes=[pltpu.SMEM(v.shape, f32) for v in notes]
        + [staging, staging, sem((rows,)), sem((rows,)), sem((n + 1,))]
        + [pltpu.VMEM((rows, 128), f32), pltpu.SMEM((8, 128), f32)]
        + solve_scratch(extent, rows),
        compiler_params=params,
        name="solve_target",
    )(*notes, *[in_vmem(v) for v in raw], upper, plan, *fixed)
    goals = pltpu.with_memory_space_constraint(goals, pltpu.SMEM)
    moved = pl.pallas_call(
        lambda *refs: place_kernel(lay, *refs),
        out_shape=pltpu.HBM(plastic.shape, f32),
        in_specs=[smem] + [vmem] * (n + 1) + [anywhere],
        out_specs=anywhere,
        scratch_shapes=[sem((total,))],
        input_output_aliases={n + 2: 0},
        compiler_params=params,
        name="place",
    )(goals, *[in_vmem(v) for v in done], in_vmem(finished), in_hbm(arrived))
    moved = lax.cond(rare[0] > 0, unusual, lambda v: v, moved)
    return force, moved


def solution(mesh):
    everyone = ("rve", "mic", "mac")

    return jax.shard_map(
        on_device,
        mesh=mesh,
        in_specs=(
            P(None, "rve", ("mic", "mac"), None),
            P(everyone, None, None, None),
            P(), P(), P(),
            P(everyone),
            P(everyone),
        ),
        out_specs=(P(None, "rve", ("mic", "mac"), None), P(everyone, None, None, None)),
        check_vma=False,
    )
```

```python
import math

import jax
import jax.numpy as jnp
import numpy as np
from jax import lax
from jax.experimental import pallas as pl
from jax.experimental.pallas import tpu as pltpu
from jax.sharding import PartitionSpec as P


COUPLING = 0.7
EARLY = 2
VMEM_BYTES = 20 * 2**20
SMALL_BYTES = 8 * 2**20
PAIRS = [(0, 0), (1, 1), (2, 2), (1, 2), (0, 2), (0, 1)]
SYM = [(m, n) for m in range(6) for n in range(m, 6)]


def symbol_table(extent):
    wave = ((np.arange(extent) + extent // 2) % extent - extent // 2).astype(np.float64)
    grid = np.meshgrid(wave, wave, wave, indexing="ij")
    square = grid[0] ** 2 + grid[1] ** 2 + grid[2] ** 2
    live = square > 0
    safe = np.where(live, square, 1.0)
    full = np.zeros((6, 6) + square.shape)
    for n, (p, q) in enumerate(PAIRS):
        traction = [np.zeros_like(square) for _ in range(3)]
        traction[p] = traction[p] + grid[q]
        if p != q:
            traction[q] = traction[q] + grid[p]
        normal = sum(grid[i] * traction[i] for i in range(3))
        weight = 1.0 if p == q else 2.0
        for m, (i, j) in enumerate(PAIRS):
            value = (grid[j] * traction[i] + grid[i] * traction[j]) / (2.0 * safe)
            value = value - COUPLING * grid[i] * grid[j] * normal / safe**2
            full[m, n] = np.where(live, value, 0.0) / weight
    flip = (-np.arange(extent)) % extent
    mirrored = full[:, :, flip][:, :, :, flip][:, :, :, :, flip]
    real = 0.5 * (full + mirrored) / extent**3
    half = extent // 2
    scale = np.where((np.arange(half + 1) % half) == 0, 1.0, 2.0).reshape(-1, 1)
    table = np.zeros((len(SYM), extent, extent * extent))
    for index, (m, n) in enumerate(SYM):
        table[index, : half + 1] = real[m, n, : half + 1].reshape(half + 1, -1) * scale
    return table.astype(np.float32)


def plane_tables(extent):
    plane = np.arange(extent * extent)
    row, col = plane // extent, plane % extent
    phase = (row[:, None] * row[None, :] + col[:, None] * col[None, :]) % extent
    angle = 2.0 * np.pi * phase / extent
    out = []
    for value in (np.cos(angle) + np.sin(angle), np.cos(angle) - np.sin(angle)):
        value = value.astype(np.float32)
        high = value.astype(jnp.bfloat16)
        low = (value - high.astype(np.float32)).astype(jnp.bfloat16)
        out.append(np.concatenate([high, high, low], axis=0))
    return np.stack(out)


C1, C2, C3 = math.cos(math.pi / 8), math.cos(math.pi / 4), math.cos(3 * math.pi / 8)


def cosine_sums(first, s, last):
    p = [s[j - 1] + s[7 - j] for j in (1, 2, 3)]
    m = [s[j - 1] - s[7 - j] for j in (1, 2, 3)]
    mid = s[3]
    total, diff = first + last, first - last
    t = m[1] * C2
    u, v = diff + t, diff - t
    w1 = m[0] * C1 + m[2] * C3
    w3 = m[0] * C3 - m[2] * C1
    plus, minus = total + mid, total - mid
    outer, inner = p[0] + p[2], (p[0] - p[2]) * C2
    even = plus + p[1]
    return [
        even + outer, u + w1, minus + inner, v + w3, plus - p[1],
        v - w3, minus - inner, u - w1, even - outer,
    ]


def sine_sums(d):
    n = [d[j - 1] + d[7 - j] for j in (1, 2, 3)]
    r = [d[j - 1] - d[7 - j] for j in (1, 2, 3)]
    mid = d[3]
    y1 = n[0] * C3 + n[2] * C1
    y3 = n[0] * C1 - n[2] * C3
    g = n[1] * C2
    gp, gm = g + mid, g - mid
    e = (r[0] + r[2]) * C2
    return [y1 + gp, e + r[1], y3 + gm, r[0] - r[2], y3 - gm, e - r[1], y1 - gp]


def split_dot(x, weights):
    high = x.astype(jnp.bfloat16)
    low = (x - high.astype(jnp.float32)).astype(jnp.bfloat16)
    stacked = jnp.concatenate([high, low, high], axis=1)
    return jnp.dot(stacked, weights, preferred_element_type=jnp.float32)


def elastic_parts(strain, plastic, shear2):
    elastic = [strain[c] - plastic[c] for c in range(6)]
    volume = elastic[0] + elastic[1] + elastic[2]
    mean = volume * (1.0 / 3.0)
    dev = [elastic[c] - mean for c in range(3)] + elastic[3:]
    normal = dev[0] * dev[0] + dev[1] * dev[1] + dev[2] * dev[2]
    shear = dev[3] * dev[3] + dev[4] * dev[4] + dev[5] * dev[5]
    size = (normal + (shear + shear)) * (shear2 * shear2)
    return volume, dev, size


def solve(extent, rows, state, out, strain_cols, late_counts, consts, scratch, ship=None):
    table_ref, plane_ref = consts
    bulk_ref, shear_ref, radius_ref = [table_ref.at[len(SYM) + i] for i in range(3)]
    e_ref, u_ref, a_ref, b_ref, a2_ref, b2_ref, t_ref = scratch
    half = extent // 2
    wide = extent * extent
    lanes = 128
    group = 6 * rows

    for c in range(6):
        column = jnp.broadcast_to(strain_cols[c], (rows, wide))
        for a in range(extent):
            e_ref[c, a] = column
            u_ref[0, c, a] = jnp.zeros((rows, wide), jnp.float32)
            u_ref[1, c, a] = jnp.zeros((rows, wide), jnp.float32)
    count_col, top_count = late_counts()

    def current(a, tile, k, alpha, beta):
        lane = pl.ds(tile * lanes, lanes)
        newer, older = (k + 1) & 1, k & 1
        values = []
        for c in range(6):
            v = e_ref[c, a, :, lane] - alpha * u_ref[newer, c, a, :, lane]
            values.append(v - beta * u_ref[older, c, a, :, lane])
        plastic = [state[c, a, :, lane] for c in range(6)]
        shear2 = 2.0 * shear_ref[pl.ds(a, 1), lane]
        radius = radius_ref[pl.ds(a, 1), lane]
        bulk = bulk_ref[pl.ds(a, 1), lane]
        volume, dev, size = elastic_parts(values, plastic, shear2)
        factor = radius * lax.rsqrt(jnp.maximum(size, radius * radius))
        gain = factor * shear2
        pressure = bulk * volume
        stress = [gain * dev[c] + pressure for c in range(3)]
        stress += [gain * dev[c] for c in range(3, 6)]
        return values, plastic, dev, factor, stress

    def sweep(k, carry):
        alpha, beta, before = carry
        for a in range(extent):
            for tile in range(wide // lanes):
                lane = pl.ds(tile * lanes, lanes)
                values, _, _, _, stress = current(a, tile, k, alpha, beta)
                for c in range(6):
                    e_ref[c, a, :, lane] = values[c]
                    t_ref[c, a, :, lane] = stress[c]
        for c in range(6):
            for tile in range(wide // lanes):
                lane = pl.ds(tile * lanes, lanes)
                x = [t_ref[c, a, :, lane] for a in range(extent)]
                s = [x[j] + x[extent - j] for j in range(1, half)]
                d = [x[j] - x[extent - j] for j in range(1, half)]
                for kk, value in enumerate(cosine_sums(x[0], s, x[half])):
                    a_ref[pl.ds(kk * group + c * rows, rows), lane] = value
                for kk, value in enumerate(sine_sums(d)):
                    b_ref[pl.ds(kk * group + c * rows, rows), lane] = value
        a2_ref[...] = split_dot(a_ref[...], plane_ref[0])
        b2_ref[...] = split_dot(b_ref[...], plane_ref[1])
        for kk in range(half + 1):
            ends = kk == 0 or kk == half
            for tile in range(wide // lanes):
                lane = pl.ds(tile * lanes, lanes)
                coef = {}
                for index, pair in enumerate(SYM):
                    coef[pair] = table_ref[index, pl.ds(kk, 1), lane]
                    coef[pair[::-1]] = coef[pair]

                def place(c, odd):
                    if ends:
                        return a2_ref, a_ref, pl.ds(kk * group + c * rows, rows)
                    if (c >= 4) != odd:
                        return b2_ref, b_ref, pl.ds((kk - 1) * group + c * rows, rows)
                    return a2_ref, a_ref, pl.ds(kk * group + c * rows, rows)

                for odd in (False,) if ends else (False, True):
                    tau = []
                    for c in range(6):
                        src, _, where = place(c, odd)
                        value = src[where, lane]
                        tau.append(value if c < 3 else value + value)
                    for m in range(6):
                        acc = coef[m, 0] * tau[0]
                        for n in range(1, 6):
                            acc = acc + coef[m, n] * tau[n]
                        _, dst, where = place(m, odd)
                        dst[where, lane] = acc
        a2_ref[...] = split_dot(a_ref[...], plane_ref[0])
        b2_ref[...] = split_dot(b_ref[...], plane_ref[1])
        num = jnp.zeros((rows, lanes), jnp.float32)
        den = jnp.zeros((rows, lanes), jnp.float32)
        newest, last = k & 1, (k + 1) & 1
        for c in range(6):
            for tile in range(wide // lanes):
                lane = pl.ds(tile * lanes, lanes)
                ca = [a2_ref[pl.ds(kk * group + c * rows, rows), lane] for kk in range(half + 1)]
                sb = [b2_ref[pl.ds(kk * group + c * rows, rows), lane] for kk in range(half - 1)]
                even = cosine_sums(ca[0], ca[1:half], ca[half])
                odd = [None] + sine_sums(sb)
                for a in range(extent):
                    j = min(a, extent - a)
                    if a == 0 or a == half:
                        value = even[j]
                    elif a < half:
                        value = even[j] + odd[j]
                    else:
                        value = even[j] - odd[j]
                    change = value - u_ref[last, c, a, :, lane]
                    num = num + change * value
                    den = den + change * change
                    u_ref[newest, c, a, :, lane] = value
        scale = 1.0 / (6 * extent**3)
        top = jnp.sum(num, axis=1, keepdims=True) * scale
        bottom = jnp.sum(den, axis=1, keepdims=True) * scale + 1e-06
        weight = jnp.where(k > 0, top / bottom, 0.0)
        active = jnp.where(count_col > k.astype(jnp.float32), 1.0, 0.0)
        alpha = active * (1.0 - weight)
        beta = active * weight * before
        spread = lambda v: jnp.broadcast_to(v, (rows, lanes))
        return spread(alpha), spread(beta), weight

    zero = jnp.zeros((rows, lanes), jnp.float32)
    alpha, beta, _ = lax.fori_loop(
        0, top_count, sweep, (zero, zero, jnp.zeros((rows, 1), jnp.float32))
    )
    sums = [jnp.zeros((rows, lanes), jnp.float32) for _ in range(6)]
    for a in range(extent):
        for tile in range(wide // lanes):
            lane = pl.ds(tile * lanes, lanes)
            _, plastic, dev, factor, stress = current(a, tile, top_count, alpha, beta)
            rest = 1.0 - factor
            for c in range(6):
                sums[c] = sums[c] + stress[c]
                out[c, a, :, lane] = plastic[c] + rest * dev[c]
        if ship and a % half == half - 1:
            ship(a // half)
    return sums


def solve_scratch(extent, rows):
    half, wide = extent // 2, extent * extent
    field = (6, extent, rows, wide)
    f32 = jnp.float32
    return [
        pltpu.VMEM(field, f32),
        pltpu.VMEM((2,) + field, f32),
        pltpu.VMEM(((half + 1) * 6 * rows, wide), f32),
        pltpu.VMEM(((half - 1) * 6 * rows, wide), f32),
        pltpu.VMEM(((half + 1) * 6 * rows, wide), f32),
        pltpu.VMEM(((half - 1) * 6 * rows, wide), f32),
        pltpu.VMEM(field, f32),
    ]


def to_column(row, mask):
    return jnp.sum(jnp.where(mask, jnp.broadcast_to(row, mask.shape), 0.0), axis=1, keepdims=True)


def to_row(column, mask):
    return jnp.sum(jnp.where(mask, jnp.broadcast_to(column, mask.shape), 0.0), axis=0, keepdims=True)


def counts_column(counts, rows):
    where = lax.broadcasted_iota(jnp.int32, (rows, 1), 0)
    column = jnp.zeros((rows, 1), jnp.float32)
    top = counts[0]
    for r in range(rows):
        column = jnp.where(where == r, counts[r].astype(jnp.float32), column)
        top = jnp.maximum(top, counts[r])
    return column, top


def lane_mask(rows):
    shape = (rows, 128)
    return lax.broadcasted_iota(jnp.int32, shape, 0) == lax.broadcasted_iota(jnp.int32, shape, 1)


def spread_nodes(value):
    return value, pltpu.roll(value, 127, 1)


def strain_rows(corners):
    pairs = [spread_nodes(v) for v in corners]
    total = [lo + hi for lo, hi in pairs]
    rise = [hi - lo for lo, hi in pairs]
    h = [
        0.25 * ((total[1] + total[3]) - (total[0] + total[2])),
        0.25 * ((total[2] + total[3]) - (total[0] + total[1])),
        0.25 * ((rise[0] + rise[1]) + (rise[2] + rise[3])),
    ]
    pick = lambda i, j: h[j][i : i + 1]
    return [
        pick(0, 0), pick(1, 1), pick(2, 2),
        0.5 * (pick(1, 2) + pick(2, 1)),
        0.5 * (pick(0, 2) + pick(2, 0)),
        0.5 * (pick(0, 1) + pick(1, 0)),
    ]


def zero_below(value):
    return value, pltpu.roll(value, 1, 1)


def node_force(own, low_a, low_b, low_ab):
    total, rise = [], []
    for value in (own, low_a, low_b, low_ab):
        value, below = zero_below(value)
        total.append(value + below)
        rise.append(below - value)
    along = [
        (total[1] + total[3]) - (total[0] + total[2]),
        (total[2] + total[3]) - (total[0] + total[1]),
        (rise[0] + rise[1]) + (rise[2] + rise[3]),
    ]
    index = [[0, 5, 4], [5, 1, 3], [4, 3, 2]]
    rows = []
    for i in range(3):
        parts = [along[j][index[i][j] : index[i][j] + 1] for j in range(3)]
        rows.append(0.25 * (parts[0] + parts[1] + parts[2]))
    return rows


class Layout:
    def __init__(self, plastic_shape, depth, layers, columns):
        self.rows, _, self.extent, self.wide = plastic_shape
        self.depth, self.layers, self.columns = depth, layers, columns
        self.peers = min(layers // 2, self.rows // 2)
        self.capacity = self.rows // self.peers
        self.near = [k for k in (1, 2) if k < layers]
        self.early = (self.capacity * EARLY) // 4
        self.late = self.capacity - self.early
        self.row = (6, self.extent, self.wide)
        self.field = (6, self.extent, self.rows, self.wide)
        self.meta = -(-self.capacity // 8) * 8

    def route(self, plan):
        here = lax.axis_index("rve")
        block = self.rows * self.columns
        partner = [lax.div(plan[e], block) for e in range(self.rows)]
        away = []
        for p in partner:
            d = p - here
            away.append(jnp.where(d < 0, d + self.layers, d))
        order = []
        for e in range(self.rows):
            before = jnp.int32(0)
            for f in range(e):
                before = before + (away[f] == away[e]).astype(jnp.int32)
            order.append(before)
        target = [lax.rem(plan[e], self.rows) for e in range(self.rows)]
        return away, order, target

    def late_slots(self):
        places = range(self.early, self.capacity)
        return [(i, s) for i in range(len(self.near)) for s in places]

    def pick(self, away, order, offset, place):
        row, found = jnp.int32(0), jnp.int32(0)
        for e in range(self.rows):
            hit = jnp.logical_and(away[e] == offset, order[e] == place)
            row = jnp.where(hit, e, row)
            found = jnp.where(hit, 1, found)
        return row, found


def pack_kernel(lay, *refs):
    displacement, plan, counts, plastic = refs[:4]
    nodes, plan_s, counts_s = refs[4:7]
    boxes = refs[7 : 7 + len(lay.near)]
    corner, small_sems, box_sems = refs[7 + len(lay.near) :]
    load_plan = pltpu.make_async_copy(plan, plan_s, small_sems.at[0])
    load_plan.start()
    load_corner = pltpu.make_async_copy(displacement, corner, small_sems.at[1])
    load_corner.start()
    load_counts = pltpu.make_async_copy(counts, counts_s, small_sems.at[2])
    load_counts.start()
    nodes[...] = jnp.zeros(nodes.shape, jnp.float32)
    load_plan.wait()
    away, order, _ = lay.route(plan_s)
    packed = []
    for i, offset in enumerate(lay.near):
        for s in range(lay.early):
            row, _ = lay.pick(away, order, offset, s)
            packed.append(pltpu.make_async_copy(plastic.at[row], boxes[i].at[s], box_sems.at[i, s]))
            packed[-1].start()
    load_corner.wait()
    for i in range(3):
        nodes[i : i + 1, : lay.depth] = corner[i, 0]
    rare = jnp.int32(0)
    for e in range(lay.rows):
        usual = away[e] == 0
        for offset in lay.near:
            usual = jnp.logical_or(usual, away[e] == offset)
        rare = jnp.where(usual, rare, 1)
    nodes[3:4] = jnp.full((1, 128), rare.astype(jnp.float32))
    load_counts.wait()
    for copy in packed:
        copy.wait()


def load_kernel(lay, *refs):
    plastic, plane, table, *fields = refs[:6]
    state, plane_copy, board = refs[6:9]
    fix_sems, row_sems = refs[9:]
    copies = []
    for r in range(lay.rows):
        copies.append(pltpu.make_async_copy(plastic.at[r], state.at[:, :, r, :], row_sems.at[r]))
    fixed = [(plane, plane_copy), (table, board.at[pl.ds(0, len(SYM))])]
    fixed += [(field, board.at[len(SYM) + i]) for i, field in enumerate(fields)]
    for i, (src, dst) in enumerate(fixed):
        copies.append(pltpu.make_async_copy(src, dst, fix_sems.at[i]))
    for copy in copies:
        copy.start()
    for copy in copies:
        copy.wait()


def source_kernel(lay, *refs):
    extent, rows = lay.extent, lay.rows
    own, upper, side, counts_s, plan_s, state, plane, board = refs[:8]
    n = len(lay.near)
    finished, first = refs[8:10]
    others = refs[10 : 9 + n]
    at = 9 + max(n, 1)
    boxes = refs[at : at + n]
    box_sems = refs[at + n]
    scratch = refs[at + n + 1 :]
    mask = lane_mask(rows)
    inside = jnp.where(lax.axis_index("rve") < lay.layers - 1, 1.0, 0.0)
    corners = [own[0:3], upper[0:3] * inside, side[0:3], side[8:11] * inside]
    strain = [to_column(v, mask) for v in strain_rows(corners)]
    column, top = counts_column(counts_s, rows)
    away, order, target = lay.route(plan_s)
    stores = []

    def ship(part):
        span = pl.ds(part * (extent // 2), extent // 2)
        for i, offset in enumerate(lay.near):
            for s in range(lay.late):
                row, _ = lay.pick(away, order, offset, lay.early + s)
                src = finished.at[:, span, row, :]
                dst = boxes[i].at[s, :, span, :]
                stores.append(pltpu.make_async_copy(src, dst, box_sems.at[i, s, part]))
                stores[-1].start()

    sums = solve(
        extent, rows, state, finished, strain, lambda: (column, top),
        (board, plane), scratch, ship,
    )
    lane = lax.broadcasted_iota(jnp.int32, (rows, 128), 1)
    sub = lax.broadcasted_iota(jnp.int32, (rows, 128), 0)
    card = jnp.zeros((rows, 128), jnp.float32)
    for c in range(6):
        card = jnp.where(lane == c, strain[c], card)
    card = jnp.where(lane == 6, column, card)
    for r in range(rows):
        label = (target[r] + 1).astype(jnp.float32)
        card = jnp.where(jnp.logical_and(lane == 7, sub == r), label, card)
    notes = (first,) + tuple(others)
    first[...] = jnp.zeros(first.shape, jnp.float32)
    for i, offset in enumerate(lay.near):
        base = 8 if i == 0 else 0
        if i:
            notes[i][...] = jnp.zeros(notes[i].shape, jnp.float32)
        for s in range(lay.capacity):
            row, found = lay.pick(away, order, offset, s)
            chosen = jnp.logical_and(sub == row, found > 0)
            line = jnp.sum(jnp.where(chosen, card, 0.0), axis=0, keepdims=True)
            line = jnp.where(lane[0:1] == 8, jnp.maximum(own[3:4], upper[3:4]), line)
            notes[i][base + s : base + s + 1] = line
    for c in range(6):
        mean = jnp.sum(sums[c], axis=1, keepdims=True) * (1.0 / extent**3)
        first[c : c + 1] = to_row(mean, mask)
    for copy in stores:
        copy.wait()


def note_row(i, s):
    return (8 if i == 0 else 0) + s


def target_kernel(lay, *refs):
    extent, rows, n = lay.extent, lay.rows, len(lay.near)
    notes, boxes = refs[:n], refs[n : 2 * n]
    upper, plan_s, plane, board = refs[2 * n : 2 * n + 4]
    arrived, rare_out, goals = refs[2 * n + 4 : 2 * n + 7]
    rest = refs[2 * n + 7 :]
    marks, rest = rest[:n], rest[n:]
    stage, result, load_sems, store_sems, mark_sems, cards, upper_s = rest[:7]
    scratch = rest[7:]
    slots = [(i, s) for i in range(n) for s in range(lay.early)]
    reads = [pltpu.make_async_copy(notes[i], marks[i], mark_sems.at[i]) for i in range(n)]
    reads.append(pltpu.make_async_copy(upper, upper_s, mark_sems.at[n]))
    loads = []
    for r, (i, s) in enumerate(slots):
        dst = stage.at[:, :, r, :]
        loads.append(pltpu.make_async_copy(boxes[i].at[s], dst, load_sems.at[r]))
    for copy in reads + loads:
        copy.start()
    cards[...] = jnp.zeros(cards.shape, jnp.float32)
    for r, (i, s) in enumerate(slots):
        cards[r : r + 1] = notes[i][note_row(i, s) : note_row(i, s) + 1]
    card = cards[...]
    strain = [card[:, c : c + 1] for c in range(6)]

    def late_counts():
        for copy in reads:
            copy.wait()
        most = jnp.float32(0.0)
        for i, s in slots:
            most = jnp.maximum(most, marks[i][note_row(i, s), 6])
        away, _, target = lay.route(plan_s)
        for index, (i, s) in enumerate(lay.late_slots()):
            goals[index] = marks[i][note_row(i, s), 7].astype(jnp.int32) - 1
        for e in range(rows):
            goals[n * lay.late + e] = jnp.where(away[e] == 0, target[e], -1)
        rare = jnp.maximum(marks[0][note_row(0, 0), 8], marks[n - 1][note_row(n - 1, 0), 8])
        rare_out[0] = jnp.where(jnp.maximum(rare, upper_s[3, 0]) > 0.0, 1, 0)
        return card[:, 6:7], most.astype(jnp.int32)

    for copy in loads:
        copy.wait()
    solve(
        extent, rows, stage, result, strain, late_counts,
        (board, plane), scratch,
    )
    moves = []
    for r, (i, s) in enumerate(slots):
        label = marks[i][note_row(i, s), 7].astype(jnp.int32)
        moves.append((r, label > 0, jnp.maximum(label - 1, 0)))
    for phase in ("start", "wait"):
        for r, valid, where in moves:

            @pl.when(valid)
            def _(r=r, where=where, phase=phase):
                src = result.at[:, :, r, :]
                copy = pltpu.make_async_copy(src, arrived.at[where], store_sems.at[r])
                getattr(copy, phase)()


def place_kernel(lay, *refs):
    n = len(lay.near)
    goals, boxes = refs[0], refs[1 : n + 1]
    own, below, beside, finished, _, out, force, line, sems, line_sem = refs[n + 1 :]
    sources = [boxes[i].at[s - lay.early] for i, s in lay.late_slots()]
    sources += [finished.at[:, :, e, :] for e in range(lay.rows)]
    for phase in ("start", "wait"):
        if phase == "wait":
            force_kernel(lay, own, below, beside, line)
            send = pltpu.make_async_copy(line, force, line_sem)
            send.start()
        for index, src in enumerate(sources):

            @pl.when(goals[index] >= 0)
            def _(index=index, src=src, phase=phase):
                where = jnp.maximum(goals[index], 0)
                getattr(pltpu.make_async_copy(src, out.at[where], sems.at[index]), phase)()

    send.wait()


def force_kernel(lay, own, below, side, out):
    inside = jnp.where(lax.axis_index("rve") > 0, 1.0, 0.0)
    rows = node_force(own[0:6], below[0:6] * inside, side[0:6], side[8:14] * inside)
    for i in range(3):
        out[i, 0] = rows[i][:, : lay.depth]


def shift_pairs(counts, steps):
    pairs = []
    for flat in range(math.prod(counts)):
        at, rest = [], flat
        for size in reversed(counts):
            at.insert(0, rest % size)
            rest //= size
        to = [p + s for p, s in zip(at, steps)]
        if all(0 <= t < size for t, size in zip(to, counts)):
            target = 0
            for t, size in zip(to, counts):
                target = target * size + t
            pairs.append((flat, target))
    return pairs


def ring(value, step):
    layers = lax.axis_size("rve")
    return lax.ppermute(value, "rve", [(i, (i + step) % layers) for i in range(layers)])


def sideways(value, step):
    columns = lax.axis_size("mic") * lax.axis_size("mac")
    return lax.ppermute(value, ("mic", "mac"), shift_pairs([columns], [step]))


def route_slots(migration_plan, width_rows, capacity):
    columns = lax.axis_size("mic") * lax.axis_size("mac")
    partner = migration_plan // width_rows // columns
    target_row = migration_plan % width_rows
    shared = partner[:, None] == partner[None, :]
    positions = jnp.arange(width_rows)
    earlier = positions[:, None] > positions[None, :]
    order_within = jnp.sum((shared & earlier).astype(jnp.int32), axis=1)
    return (partner * capacity + order_within, target_row)


def move_any(rows_next, migration_plan):
    width_rows = rows_next.shape[0]
    devices_along = lax.axis_size("rve")
    peers_used = min(devices_along // 2, width_rows // 2)
    capacity = width_rows // peers_used
    total = devices_along * capacity
    slot_index, target_row = route_slots(migration_plan, width_rows, capacity)
    matches = slot_index[None, :] == jnp.arange(total)[:, None]
    source = jnp.sum(jnp.where(matches, jnp.arange(width_rows)[None, :], 0), axis=1)
    labels = jnp.sum(jnp.where(matches, target_row[None, :] + 1, 0), axis=1)
    outgoing = jnp.take(rows_next, source, axis=0)
    arrived = lax.all_to_all(outgoing, "rve", split_axis=0, concat_axis=0, tiled=True)
    tags = lax.all_to_all(labels, "rve", split_axis=0, concat_axis=0, tiled=True)
    wanted = tags[None, :] == jnp.arange(1, width_rows + 1)[:, None]
    place = jnp.sum(jnp.where(wanted, jnp.arange(total)[None, :], 0), axis=1)
    return jnp.take(arrived, place, axis=0)


def in_hbm(value):
    return pltpu.with_memory_space_constraint(value, pltpu.HBM)


def in_vmem(value):
    return pltpu.with_memory_space_constraint(value, pltpu.VMEM)


def on_device(displacement, plastic, bulk, shear, radius, counts, migration_plan):
    layers = lax.axis_size("rve")
    columns = lax.axis_size("mic") * lax.axis_size("mac")
    lay = Layout(plastic.shape, displacement.shape[3], layers, columns)
    fast = layers <= 2 + len(lay.near)
    if not fast:
        lay.near = []
    rows, extent, wide, n = lay.rows, lay.extent, lay.wide, len(lay.near)
    f32 = jnp.float32
    plane = jnp.asarray(plane_tables(extent))
    fixed = [plane, jnp.asarray(symbol_table(extent)), bulk, shear, radius]
    vmem = pl.BlockSpec(memory_space=pltpu.VMEM)
    anywhere = pl.BlockSpec(memory_space=pl.ANY)
    smem = pl.BlockSpec(memory_space=pltpu.SMEM)
    sem = pltpu.SemaphoreType.DMA
    params = pltpu.CompilerParams(vmem_limit_bytes=VMEM_BYTES)
    staging = pltpu.VMEM(lay.field, f32)
    small = pltpu.SMEM((rows,), jnp.int32)
    plan = in_hbm(migration_plan)
    nodes, plan, counts, *raw = pl.pallas_call(
        lambda *refs: pack_kernel(lay, *refs),
        out_shape=[pltpu.VMEM((8, 128), f32), small, small]
        + [pltpu.VMEM((lay.early,) + lay.row, f32)] * n,
        in_specs=[anywhere] * 4,
        out_specs=[vmem] + [smem] * 2 + [vmem] * n,
        scratch_shapes=[
            pltpu.VMEM(displacement.shape, f32),
            sem((3,)),
            sem((max(n, 1), max(lay.early, 1))),
        ],
        compiler_params=pltpu.CompilerParams(vmem_limit_bytes=SMALL_BYTES),
        name="pack",
    )(in_hbm(displacement), plan, in_hbm(counts), in_hbm(plastic))
    plan, counts = [pltpu.with_memory_space_constraint(v, pltpu.SMEM) for v in (plan, counts)]
    state, *fixed = pl.pallas_call(
        lambda *refs: load_kernel(lay, *refs),
        out_shape=[
            staging,
            pltpu.VMEM(plane.shape, plane.dtype),
            pltpu.VMEM((len(SYM) + 3, extent, wide), f32),
        ],
        in_specs=[anywhere] * 6,
        out_specs=[vmem] * 3,
        scratch_shapes=[sem((5,)), sem((rows,))],
        compiler_params=pltpu.CompilerParams(vmem_limit_bytes=SMALL_BYTES),
        name="load",
    )(in_hbm(plastic), *[in_hbm(v) for v in fixed])
    fixed = [in_vmem(v) for v in fixed]
    upper = ring(nodes, -1)
    for i, offset in enumerate(lay.near):
        raw[i] = ring(raw[i], offset)
    both = jnp.concatenate([nodes, upper], axis=0)
    side = sideways(both, -1)
    nodes, upper = in_vmem(nodes), in_vmem(upper)
    outs = [staging, pltpu.VMEM((8 + lay.meta, 128), f32)]
    outs += [pltpu.VMEM((lay.meta, 128), f32)] * (n - 1)
    outs += [pltpu.HBM((lay.late,) + lay.row, f32)] * n
    finished, *rest = pl.pallas_call(
        lambda *refs: source_kernel(lay, *refs),
        out_shape=outs,
        in_specs=[vmem] * 3 + [smem] * 2 + [vmem] * 3,
        out_specs=[vmem] * (1 + max(n, 1)) + [anywhere] * n,
        scratch_shapes=[sem((max(n, 1), max(lay.late, 1), 2))]
        + solve_scratch(extent, rows),
        compiler_params=params,
        name="solve_source",
    )(nodes, upper, in_vmem(side), counts, plan, in_vmem(state), *fixed)
    first, others, done = rest[0], rest[1:n], rest[max(n, 1) :]
    below = ring(first, 1)
    notes = [below]
    for i, offset in enumerate(lay.near[1:]):
        notes.append(ring(others[i], offset))
    for i, offset in enumerate(lay.near):
        done[i] = ring(done[i], offset)
    pair = jnp.concatenate([first[:8], below[:8]], axis=0)
    beside = sideways(pair, 1)

    def unusual(_):
        return move_any(finished.transpose(2, 0, 1, 3), migration_plan)

    sides = [in_vmem(v) for v in (first, below, beside)]
    if not fast:
        force = pl.pallas_call(
            lambda *refs: force_kernel(lay, *refs),
            out_shape=jax.ShapeDtypeStruct(displacement.shape, f32),
            in_specs=[vmem] * 3,
            out_specs=vmem,
            compiler_params=pltpu.CompilerParams(vmem_limit_bytes=SMALL_BYTES),
            name="force",
        )(*sides)
        return force, unusual(None)
    notes = [in_vmem(v) for v in notes]
    total = n * lay.late + rows
    arrived, rare, goals = pl.pallas_call(
        lambda *refs: target_kernel(lay, *refs),
        out_shape=[
            pltpu.HBM(plastic.shape, f32),
            pltpu.SMEM((1,), jnp.int32),
            pltpu.SMEM((total,), jnp.int32),
        ],
        in_specs=[vmem] * (2 * n + 1) + [smem] + [vmem] * 2,
        out_specs=[anywhere, smem, smem],
        scratch_shapes=[pltpu.SMEM(v.shape, f32) for v in notes]
        + [staging, staging, sem((rows,)), sem((rows,)), sem((n + 1,))]
        + [pltpu.VMEM((rows, 128), f32), pltpu.SMEM((8, 128), f32)]
        + solve_scratch(extent, rows),
        compiler_params=params,
        name="solve_target",
    )(*notes, *[in_vmem(v) for v in raw], upper, plan, *fixed)
    goals = pltpu.with_memory_space_constraint(goals, pltpu.SMEM)
    moved, force = pl.pallas_call(
        lambda *refs: place_kernel(lay, *refs),
        out_shape=[pltpu.HBM(plastic.shape, f32), pltpu.HBM(displacement.shape, f32)],
        in_specs=[smem] + [vmem] * (n + 4) + [anywhere],
        out_specs=[anywhere] * 2,
        scratch_shapes=[pltpu.VMEM(displacement.shape, f32), sem((total,)), sem(())],
        input_output_aliases={n + 5: 0},
        compiler_params=params,
        name="place",
    )(goals, *[in_vmem(v) for v in done], *sides, in_vmem(finished), in_hbm(arrived))
    moved = lax.cond(rare[0] > 0, unusual, lambda v: v, moved)
    return force, moved


def solution(mesh):
    everyone = ("rve", "mic", "mac")

    return jax.shard_map(
        on_device,
        mesh=mesh,
        in_specs=(
            P(None, "rve", ("mic", "mac"), None),
            P(everyone, None, None, None),
            P(), P(), P(),
            P(everyone),
            P(everyone),
        ),
        out_specs=(P(None, "rve", ("mic", "mac"), None), P(everyone, None, None, None)),
        check_vma=False,
    )
```
